128 devices in a mesh: dp: 8 (over x, core), seq: 16 (over y, z).
Axes of the slice: x: 4, y: 4, z: 4, core: 2. Of those that a mesh axis runs over, the one named last changes fastest.
Arguments:
- hidden: bfloat16 [32768, 1536], P(('dp', 'seq')), may hold values from -6 to 6
- database: bfloat16 [8, 192, 128, 896], P('dp', 'seq'), may hold values from -8 to 8
- block_home: int32 [192], replicated, may hold values from 0 to 191, as said below
- neighbours: int32 [512, 2], P(('dp', 'seq')), may hold values from 0 to 191, as said below
- neighbour_counts: int32 [512], P(('dp', 'seq')), may hold values from 1 to 2
- encoder_gain: float32 [896], replicated, may hold values from 0.25 to 1.75
- encoder_projection: bfloat16 [896, 2688], replicated, may hold values from -2 to 2
- encoder_output: bfloat16 [896, 896], replicated, may hold values from -0.1875 to 0.1875
- cross_gain: float32 [1536], replicated, may hold values from 0.25 to 1.75
- cross_query: bfloat16 [1536, 1536], replicated, may hold values from -2 to 2
- cross_keyvalue: bfloat16 [3072, 896], replicated, may hold values from -2 to 2
- cross_output: bfloat16 [1536, 1536], replicated, may hold values from -0.15625 to 0.15625
- cotangent: bfloat16 [32768, 1536], P(('dp', 'seq')), may hold values from -6 to 6
Outputs:
- output: bfloat16 [32768, 1536], P(('dp', 'seq'))
- keyvalue_grad: float32 [3072, 896], P('seq')
The draws below stay inside these ranges and needn't reach their ends.
Inputs may be any that keep to these rules, and one draw needn't show every extreme that they name: A permutation: block b lies at position block_home[b] of the second dimension of database. `neighbours`: the 8 ids of one device's spans name at most 2 blocks whose positions lie on the same device of seq, and exactly 2 on some device, on every device. Ids may repeat.
All inputs are finite; a program needn't handle non-finite values.
Results may differ from the reference program's by a relative error of at most 0.02.
Values may be sent and summed in bfloat16 or wider, within the bound.
No kernel may reach another device: no remote copies, remote signals or barrier semaphores. Data moves between devices by JAX's collectives and lax.ppermute only.
A program may use at most 128 MiB of HBM per device.

```python
import jax
import jax.numpy as jnp
from jax import lax

D = 1536
E = 896
HEAD = 128
K = 2
SPAN = 64
BLOCK = 128
TOK_DEV = 256
SPANS_DEV = 4
CAP = 2
DB_DEV = 12
DB_BLOCKS = 192
TOKENS = 32768
SPANS = 512
N_DP = 8
N_SEQ = 16


def plan_blocks(key):
    block_home = jax.random.permutation(jax.random.fold_in(key, 11), DB_BLOCKS).astype(jnp.int32)
    inverse = jnp.argsort(block_home).astype(jnp.int32)
    readers = N_DP * N_SEQ
    requests = K * SPANS_DEV
    popular = jax.random.randint(jax.random.fold_in(key, 12), (N_SEQ,), 0, 4)
    noise = jax.random.randint(jax.random.fold_in(key, 13), (readers, N_SEQ), 0, 4 * N_SEQ)
    ranking = (noise + 3 * N_SEQ * popular[None, :]) * N_SEQ + jnp.arange(N_SEQ)[None, :]
    ranked = jnp.argsort(-ranking, axis=1).astype(jnp.int32)
    request_order = jnp.arange(requests)
    rank_pick = jnp.where(request_order < CAP, 0, 1 + (request_order - CAP) % (N_SEQ - 1))
    owners = jnp.take_along_axis(ranked, jnp.broadcast_to(rank_pick[None, :], (readers, requests)), axis=1)
    slots = jax.random.randint(jax.random.fold_in(key, 14), (readers, requests), 0, DB_DEV)
    chosen = inverse[owners * DB_DEV + slots]
    mixing = jax.random.randint(jax.random.fold_in(key, 15), (readers, requests), 0, requests * requests) * requests + request_order[None, :]
    shuffle = jnp.argsort(mixing, axis=1)
    chosen = jnp.take_along_axis(chosen, shuffle, axis=1)
    return (block_home, chosen.reshape(SPANS, K).astype(jnp.int32))


def draw_block_home(key, part):
    return plan_blocks(key)[0]


def draw_neighbours(key, part):
    return plan_blocks(key)[1]


def draw_hidden(key, part):
    values = jax.random.normal(jax.random.fold_in(key, 41), (TOKENS, D), jnp.float32)
    return jnp.clip(values, -6.0, 6.0).astype(jnp.bfloat16)


def draw_database(key, part):
    values = jax.random.normal(jax.random.fold_in(key, 51), (N_DP, DB_BLOCKS, BLOCK, E), jnp.float32)
    return jnp.clip(values, -8.0, 8.0).astype(jnp.bfloat16)


def draw_encoder_projection(key, part):
    values = jnp.clip(jax.random.normal(jax.random.fold_in(key, 61), (E, 3 * E), jnp.float32), -6.0, 6.0) * E ** (-0.5)
    return jnp.clip(values, -2.0, 2.0).astype(jnp.bfloat16)


def draw_cross_query(key, part):
    values = jnp.clip(jax.random.normal(jax.random.fold_in(key, 71), (D, D), jnp.float32), -6.0, 6.0) * D ** (-0.5)
    return jnp.clip(values, -2.0, 2.0).astype(jnp.bfloat16)


def draw_cross_keyvalue(key, part):
    values = jnp.clip(jax.random.normal(jax.random.fold_in(key, 81), (2 * D, E), jnp.float32), -6.0, 6.0) * E ** (-0.5)
    return jnp.clip(values, -2.0, 2.0).astype(jnp.bfloat16)


def plant(entries, own_key, smallest, high):
    shape = entries.shape
    index_at = [jax.random.randint(jax.random.fold_in(own_key, axis), (), 0, shape[axis]) for axis in range(len(shape))]
    entries = entries.at[tuple(index_at)].set(smallest)
    longest = shape.index(max(shape))
    index_at[longest] = (index_at[longest] + 1) % shape[longest]
    return entries.at[tuple(index_at)].set(high)


def block_scale(stream_key, shape, cuts, least, top_value):
    level = 1.0
    for dim, parts in cuts:
        draws = jax.random.uniform(jax.random.fold_in(jax.random.fold_in(stream_key, 6), dim), (parts,), jnp.float32, least / len(cuts), top_value / len(cuts))
        level = level * jnp.repeat(jnp.exp(draws), shape[dim] // parts).reshape((-1,) + (1,) * (len(shape) - 1 - dim))
    return level


def gaussian(key, extent, scale, bound, pieces=(), kind=jnp.bfloat16):
    entries = jax.random.normal(key, extent, jnp.float32) * scale
    if len(pieces) > 0:
        entries = block_scale(key, extent, pieces, -0.22, 0.18) * entries
    return jnp.clip(entries, min=-bound, max=bound).astype(kind)


def setup_inputs(seed: int = 0) -> dict:
    seeds = jax.random.split(jax.random.key(seed), 14)
    return {
        "hidden": draw_hidden(jax.random.fold_in(seeds[13], 71), 0),
        "database": draw_database(jax.random.fold_in(seeds[13], 71), 0),
        "block_home": draw_block_home(jax.random.fold_in(seeds[13], 71), 0),
        "neighbours": draw_neighbours(jax.random.fold_in(seeds[13], 71), 0),
        "neighbour_counts": plant(jax.random.randint(seeds[4], (SPANS,), 1, K + 1), jax.random.fold_in(seeds[4], 1), 1, K).astype(jnp.int32),
        "encoder_gain": jnp.clip(1.0 + 0.15 * jax.random.normal(seeds[5], (E,), jnp.float32), 0.25, 1.75),
        "encoder_projection": draw_encoder_projection(jax.random.fold_in(seeds[13], 71), 0),
        "encoder_output": gaussian(seeds[7], (E, E), E ** -0.5, 0.1875),
        "cross_gain": jnp.clip(1.0 + 0.15 * jax.random.normal(seeds[8], (D,), jnp.float32), 0.25, 1.75),
        "cross_query": draw_cross_query(jax.random.fold_in(seeds[13], 71), 0),
        "cross_keyvalue": draw_cross_keyvalue(jax.random.fold_in(seeds[13], 71), 0),
        "cross_output": gaussian(seeds[11], (D, D), D ** -0.5, 0.15625),
        "cotangent": gaussian(seeds[12], (TOKENS, D), 1.0, 6.0, ((0, 128),)),
    }


EPSILON = 1e-06

def rounded(values):
    return lax.optimization_barrier(values.astype(jnp.bfloat16)).astype(jnp.float32)

def rms_norm(values, norm_gain):
    widened = values.astype(jnp.float32)
    return widened * lax.rsqrt(lax.optimization_barrier(jnp.mean(widened * widened, axis=-1, keepdims=True)) + EPSILON) * norm_gain

def encode(blocks, encoder_gain, encoder_projection, encoder_output):
    count, length, width = blocks.shape
    head_count = width // HEAD
    normed = rms_norm(blocks, encoder_gain).astype(jnp.bfloat16)
    projected = jnp.dot(normed.reshape(count * length, width), encoder_projection, preferred_element_type=jnp.float32)
    projected = rounded(projected).reshape(count, length, 3, head_count, HEAD)
    scores = jnp.einsum('bqhd,bkhd->bhqk', projected[:, :, 0], projected[:, :, 1]) * HEAD ** (-0.5)
    weights = rounded(jax.nn.softmax(scores, axis=-1))
    attended = jnp.einsum('bhqk,bkhd->bqhd', weights, projected[:, :, 2]).astype(jnp.bfloat16)
    mixed = jnp.dot(attended.reshape(count * length, width), encoder_output, preferred_element_type=jnp.float32)
    return (blocks.astype(jnp.float32) + mixed.reshape(count, length, width)).astype(jnp.bfloat16)

def attend(queries, keyvalue, key_mask, row_flag, grad_attended):
    groups, rows, width = queries.shape
    key_total = keyvalue.shape[1]
    head_count = width // HEAD
    score_scale = HEAD ** (-0.5)
    query_heads = queries.astype(jnp.float32).reshape(groups, rows, head_count, HEAD)
    key_heads = keyvalue[:, :, :width].astype(jnp.float32).reshape(groups, key_total, head_count, HEAD)
    value_heads = keyvalue[:, :, width:].astype(jnp.float32).reshape(groups, key_total, head_count, HEAD)
    grad_heads = grad_attended.astype(jnp.float32).reshape(groups, rows, head_count, HEAD)
    scores = jnp.einsum('gqhd,gkhd->ghqk', query_heads, key_heads) * score_scale
    scores = jnp.where(key_mask[:, None, None, :], scores, -1e+30)
    chances = jax.nn.softmax(scores, axis=-1) * row_flag[:, None, :, None]
    chances_low = rounded(chances)
    attended = jnp.einsum('ghqk,gkhd->gqhd', chances_low, value_heads).astype(jnp.bfloat16)
    grad_chances = jnp.einsum('gqhd,gkhd->ghqk', grad_heads, value_heads)
    grad_scores = rounded(chances * (grad_chances - lax.optimization_barrier(jnp.sum(chances * grad_chances, axis=-1, keepdims=True))))
    grad_keys = jnp.einsum('ghqk,gqhd->gkhd', grad_scores, query_heads) * score_scale
    grad_values = jnp.einsum('ghqk,gqhd->gkhd', chances_low, grad_heads)
    grad_keyvalue = jnp.concatenate([grad_keys.reshape(groups, key_total, width), grad_values.reshape(groups, key_total, width)], axis=-1).astype(jnp.bfloat16)
    return (attended.reshape(groups, rows, width), grad_keyvalue)

def reference(hidden, database, block_home, neighbours, neighbour_counts, encoder_gain, encoder_projection, encoder_output, cross_gain, cross_query, cross_keyvalue, cross_output, cotangent):
    seq_length = TOK_DEV * N_SEQ
    span_total = seq_length // SPAN
    width = hidden.shape[1]
    feature = database.shape[3]
    normed = rms_norm(hidden, cross_gain).astype(jnp.bfloat16)
    queries = jnp.dot(normed, cross_query, preferred_element_type=jnp.float32).astype(jnp.bfloat16)
    grad_attended = lax.dot_general(cotangent, cross_output, (((1,), (1,)), ((), ())), preferred_element_type=jnp.float32).astype(jnp.bfloat16)

    def shifted(values):
        rows = values.reshape(N_DP, seq_length, width)
        moved = jnp.concatenate([rows[:, SPAN - 1:], jnp.zeros((N_DP, SPAN - 1, width), values.dtype)], axis=1)
        return moved.reshape(N_DP * span_total, SPAN, width)
    query_spans = shifted(queries)
    grad_spans = shifted(grad_attended)
    positions = block_home[neighbours].reshape(N_DP * span_total, K).astype(jnp.int32)
    row_index = (jnp.arange(N_DP * span_total) // span_total).astype(jnp.int32)

    def step(total, inputs):
        row, position, count, query_block, grad_block = inputs
        blocks = database[row][position]
        encoded = encode(blocks, encoder_gain, encoder_projection, encoder_output)
        key_rows = encoded.reshape(K * BLOCK, feature)
        keyvalue = lax.dot_general(key_rows, cross_keyvalue, (((1,), (1,)), ((), ())), preferred_element_type=jnp.float32).astype(jnp.bfloat16)
        key_mask = jnp.arange(K * BLOCK) // BLOCK < count
        attended, grad_keyvalue = attend(query_block[None], keyvalue[None], key_mask[None], jnp.ones((1, SPAN), jnp.float32), grad_block[None])
        term = lax.dot_general(grad_keyvalue[0], key_rows, (((0,), (0,)), ((), ())), preferred_element_type=jnp.float32)
        return (total + term, attended[0])
    start = jnp.zeros((2 * width, feature), jnp.float32)
    keyvalue_grad, attended_spans = lax.scan(step, start, (row_index, positions, neighbour_counts, query_spans, grad_spans))
    attended = attended_spans.reshape(N_DP, seq_length, width)
    attended = jnp.concatenate([jnp.zeros((N_DP, SPAN - 1, width), jnp.bfloat16), attended[:, :seq_length - SPAN + 1]], axis=1).reshape(-1, width)
    cross = jnp.dot(attended, cross_output, preferred_element_type=jnp.float32)
    output = (hidden.astype(jnp.float32) + cross).astype(jnp.bfloat16)
    return (output, keyvalue_grad)
```

```python
import functools

import jax
import jax.numpy as jnp
from jax import lax
from jax.experimental import pallas as pl
from jax.experimental.pallas import tpu as pltpu
from jax.sharding import PartitionSpec as P


HEAD = 128
K = 2
SPAN = 64
EPSILON = 1e-06
BF16 = jnp.bfloat16
F32 = jnp.float32
VMEM = pltpu.VMEM
NN = (((1,), (0,)), ((), ()))
NT = (((1,), (1,)), ((), ()))
TN = (((0,), (0,)), ((), ()))


def dot(a, b, dims):
    return lax.dot_general(a, b, dims, preferred_element_type=F32)


def rms_norm(values, norm_gain):
    widened = values.astype(F32)
    return (
        widened
        * lax.rsqrt(jnp.mean(widened * widened, axis=-1, keepdims=True) + EPSILON)
        * norm_gain
    )


def spread_kernel(blocks_ref, notes_ref, hidden_ref, cotangent_ref, slices_ref, tails_ref):
    blocks, _, feature = blocks_ref.shape
    devices, units, rows, _ = slices_ref.shape
    tiles = feature // HEAD
    for d in range(devices):
        for b in range(blocks):
            for k in range(tiles):
                slices_ref[d, b * tiles + k] = blocks_ref[
                    b, d * rows : (d + 1) * rows, k * HEAD : (k + 1) * HEAD
                ]
        slices_ref[d, units - 1] = notes_ref[...]

    @pl.when(pl.program_id(0) == 0)
    def _():
        tails_ref[0] = hidden_ref[...]
        tails_ref[1] = cotangent_ref[...]


def spread(database, notes, hidden, cotangent, devices):
    blocks, length, feature = database.shape
    width = hidden.shape[1]
    units = blocks * (feature // HEAD) + 1
    rows = length // devices
    step = 4
    return pl.pallas_call(
        spread_kernel,
        grid=(devices // step,),
        out_shape=(
            jax.ShapeDtypeStruct((devices, units, rows, HEAD), BF16),
            jax.ShapeDtypeStruct((2, SPAN, width), BF16),
        ),
        in_specs=[
            pl.BlockSpec((blocks, step * rows, feature), lambda i: (0, i, 0)),
            pl.BlockSpec((rows, HEAD), lambda i: (0, 0)),
            pl.BlockSpec((SPAN, width), lambda i: (0, 0)),
            pl.BlockSpec((SPAN, width), lambda i: (0, 0)),
        ],
        out_specs=(
            pl.BlockSpec((step, units, rows, HEAD), lambda i: (i, 0, 0, 0)),
            pl.BlockSpec((2, SPAN, width), lambda i: (0, 0, 0)),
        ),
        cost_estimate=pl.CostEstimate(flops=1 << 20, bytes_accessed=6 << 20, transcendentals=0),
        compiler_params=pltpu.CompilerParams(vmem_limit_bytes=60 << 20),
        name="spread",
    )(database, notes, hidden, cotangent)


def pick_kernel(tiles, where_ref, table_ref, *outs):
    blocks = table_ref.shape[1] // tiles

    @pl.loop(0, outs[0].shape[0])
    def _(r):
        first = 0
        for out in outs:
            for i in range(out.shape[1] // tiles):
                where = where_ref[r, first + i]
                start = (where % blocks) * tiles
                out[r, i * tiles : (i + 1) * tiles] = table_ref[
                    where // blocks, pl.ds(start, tiles)
                ]
            first += out.shape[1] // tiles


def pick(where, table, tiles, chunks):
    readers, requests = where.shape
    rows, width = table.shape[2:]
    shape = jax.ShapeDtypeStruct((readers, requests // chunks * tiles, rows, width), BF16)
    whole = pl.BlockSpec(memory_space=VMEM)
    return pl.pallas_call(
        functools.partial(pick_kernel, tiles),
        out_shape=(shape,) * chunks,
        in_specs=[pl.BlockSpec(memory_space=pltpu.SMEM), whole],
        out_specs=(whole,) * chunks,
        compiler_params=pltpu.CompilerParams(vmem_limit_bytes=60 << 20),
        name="pick",
    )(where, table)


def span_kernel(
    first_span,
    counts_ref,
    pieces_ref,
    gain_ref,
    projection_hbm,
    output_hbm,
    keyvalue_hbm,
    queries_ref,
    grads_ref,
    encoded_ref,
    grad_ref,
    attended_ref,
    projection_ref,
    output_ref,
    keyvalue_ref,
    plain_ref,
    normed_ref,
    qkv_ref,
    mixed_ref,
    kv_ref,
    encoder_scores_ref,
    encoder_weights_ref,
    scores_ref,
    changes_ref,
    chances_ref,
    grad_scores_ref,
    sems,
):
    slices, _, rows, _ = pieces_ref.shape
    length = slices * rows
    total, feature = encoded_ref.shape
    width = queries_ref.shape[1]
    blocks = total // length
    tiles = feature // HEAD
    heads = width // HEAD
    spans = blocks // K
    keys = K * length
    scale = HEAD ** (-0.5)
    chunk = 2 * width // (slices * 8)
    tile = 512
    steps = (3 * feature) // tile
    rest = pl.ds(steps * tile, 3 * feature - steps * tile)
    wide_steps = 2 * width // tile

    def load(columns, index):
        return pltpu.make_async_copy(
            projection_hbm.at[:, columns], projection_ref.at[:, columns], sems.at[index]
        )

    def wide_load(columns, index):
        return pltpu.make_async_copy(
            keyvalue_hbm.at[columns], keyvalue_ref.at[columns], sems.at[steps + 2 + index]
        )

    output_load = pltpu.make_async_copy(output_hbm, output_ref, sems.at[steps + 1])
    for j in range(steps):
        load(pl.ds(j * tile, tile), j).start()
    load(rest, steps).start()
    output_load.start()
    for j in range(wide_steps):
        wide_load(pl.ds(j * tile, tile), j).start()

    gain = gain_ref[...].reshape(1, feature)
    for b in range(blocks):
        block_rows = slice(b * length, (b + 1) * length)
        for k in range(tiles):
            plain_ref[block_rows, k * HEAD : (k + 1) * HEAD] = (
                pieces_ref[:, b * tiles + k].astype(F32).reshape(length, HEAD)
            )
        normed_ref[block_rows] = rms_norm(plain_ref[block_rows], gain).astype(BF16)

    @pl.loop(0, steps)
    def _(j):
        columns = pl.ds(pl.multiple_of(j * tile, tile), tile)
        load(columns, j).wait()
        qkv_ref[:, columns] = dot(normed_ref[...], projection_ref[:, columns], NN).astype(BF16)

    load(rest, steps).wait()
    qkv_ref[:, rest] = dot(normed_ref[...], projection_ref[:, rest], NN).astype(BF16)

    together = 2
    ones = jnp.ones((length, HEAD), BF16)

    @pl.loop(0, blocks // together)
    def _(step):
        pairs = [(b, h) for b in range(together) for h in range(tiles)]

        def part(which, b, h):
            start = pl.multiple_of((step * together + b) * length, length)
            return qkv_ref[pl.ds(start, length), pl.ds(which * feature + h * HEAD, HEAD)]

        for i, (b, h) in enumerate(pairs):
            encoder_scores_ref[i] = dot(part(0, b, h), part(1, b, h), NT) * scale
        tops = [jnp.max(encoder_scores_ref[i], axis=-1, keepdims=True) for i in range(len(pairs))]
        for i, top in enumerate(tops):
            encoder_weights_ref[i] = jnp.exp(encoder_scores_ref[i] - top).astype(BF16)
        for i, (b, h) in enumerate(pairs):
            value = jnp.concatenate([part(2, b, h), ones], axis=-1)
            summed_up = dot(encoder_weights_ref[i], value, NN)
            start = pl.multiple_of((step * together + b) * length, length)
            mixed_ref[pl.ds(start, length), h * HEAD : (h + 1) * HEAD] = (
                summed_up[:, :HEAD] / summed_up[:, HEAD:]
            ).astype(BF16)

    output_load.wait()
    for start in range(0, feature, 256):
        columns = slice(start, min(start + 256, feature))
        encoded_ref[:, columns] = (
            plain_ref[:, columns] + dot(mixed_ref[...], output_ref[:, columns], NN)
        ).astype(BF16)

    @pl.loop(0, wide_steps)
    def _(j):
        columns = pl.ds(pl.multiple_of(j * tile, tile), tile)
        wide_load(columns, j).wait()
        kv_ref[:, columns] = dot(encoded_ref[...], keyvalue_ref[columns, :], NT).astype(BF16)

    key_block = lax.broadcasted_iota(jnp.int32, (1, keys), 1) // length

    @pl.loop(0, spans)
    def _(u):
        valid = key_block < counts_ref[first_span + u]
        query_rows = pl.ds(pl.multiple_of(u * SPAN, SPAN), SPAN)
        key_rows = pl.ds(pl.multiple_of(u * keys, keys), keys)

        def columns(h):
            return slice(h * HEAD, (h + 1) * HEAD)

        for h in range(heads):
            key = kv_ref[key_rows, columns(h)]
            value = kv_ref[key_rows, columns(heads + h)]
            scores = dot(queries_ref[query_rows, columns(h)], key, NT) * scale
            scores_ref[h] = jnp.where(valid, scores, -1e30)
            changes_ref[h] = dot(grads_ref[query_rows, columns(h)], value, NT)
        tops = [jnp.max(scores_ref[h], axis=-1, keepdims=True) for h in range(heads)]
        for h in range(heads):
            scores_ref[h] = jnp.exp(scores_ref[h] - tops[h])
        sums = [jnp.sum(scores_ref[h], axis=-1, keepdims=True) for h in range(heads)]
        for h in range(heads):
            chances = scores_ref[h] * (1.0 / sums[h])
            scores_ref[h] = chances
            chances_ref[h] = chances.astype(BF16)
        inners = [
            jnp.sum(scores_ref[h] * changes_ref[h], axis=-1, keepdims=True) for h in range(heads)
        ]
        for h in range(heads):
            grad_scores_ref[h] = (scores_ref[h] * (changes_ref[h] - inners[h])).astype(BF16)
        for h in range(heads):
            value = kv_ref[key_rows, columns(heads + h)]
            query = queries_ref[query_rows, columns(h)]
            grad = grads_ref[query_rows, columns(h)]
            attended_ref[query_rows, columns(h)] = dot(chances_ref[h], value, NN).astype(BF16)
            for part, piece in enumerate(
                (
                    dot(query, grad_scores_ref[h], TN) * scale,
                    dot(grad, chances_ref[h], TN),
                )
            ):
                for j in range(HEAD // 8):
                    row = part * width + h * HEAD + j * 8
                    seq, inside = divmod(row, 8 * chunk)
                    dp, offset = divmod(inside, chunk)
                    base = ((dp // 2) * slices + seq) * chunk + offset
                    grad_ref[dp % 2, base : base + 8, key_rows] = piece[j * 8 : j * 8 + 8].astype(
                        BF16
                    )


def span_step(part, counts, pieces, gain, projection, output, keyvalue, queries, grads):
    width = queries.shape[1]
    feature = keyvalue.shape[1]
    slices, units, rows, _ = pieces.shape
    tiles = feature // HEAD
    length = slices * rows
    blocks = units // tiles
    total = blocks * length
    spans = blocks // K
    keys = K * length
    heads = width // HEAD
    whole = pl.BlockSpec(memory_space=VMEM)
    hbm = pl.BlockSpec(memory_space=pltpu.HBM)
    own = pl.BlockSpec((spans * SPAN, width), lambda i: (part, 0))
    return pl.pallas_call(
        functools.partial(span_kernel, part * spans),
        grid=(1,),
        out_shape=(
            jax.ShapeDtypeStruct((total, feature), BF16),
            jax.ShapeDtypeStruct((2, width, total), BF16),
            jax.ShapeDtypeStruct((spans * SPAN, width), BF16),
        ),
        in_specs=[
            pl.BlockSpec(memory_space=pltpu.SMEM),
            whole,
            whole,
            hbm,
            hbm,
            hbm,
            own,
            own,
        ],
        out_specs=(whole, whole, whole),
        scratch_shapes=[
            VMEM(projection.shape, BF16),
            VMEM(output.shape, BF16),
            VMEM(keyvalue.shape, BF16),
            VMEM((total, feature), F32),
            VMEM((total, feature), BF16),
            VMEM((total, 3 * feature), BF16),
            VMEM((total, feature), BF16),
            VMEM((total, 2 * width), BF16),
            VMEM((2 * tiles, length, length), F32),
            VMEM((2 * tiles, length, length), BF16),
            VMEM((heads, SPAN, keys), F32),
            VMEM((heads, SPAN, keys), F32),
            VMEM((heads, SPAN, keys), BF16),
            VMEM((heads, SPAN, keys), BF16),
            pltpu.SemaphoreType.DMA((3 * feature // 512 + 2 + 2 * width // 512,)),
        ],
        cost_estimate=pl.CostEstimate(
            flops=total * feature * (8 * feature + 4 * width),
            bytes_accessed=20 << 20,
            transcendentals=1 << 20,
        ),
        compiler_params=pltpu.CompilerParams(vmem_limit_bytes=60 << 20),
        name="spans",
    )(counts, pieces, gain, projection, output, keyvalue, queries, grads)


def weight_kernel(half_ref, grad_a, grad_b, encoded_a, encoded_b, out_ref):
    out_ref[...] = (
        dot(grad_a[0], encoded_a[...], NN) + dot(grad_b[0], encoded_b[...], NN)
    ).astype(BF16)


def weight_half(half, grads, encodeds):
    _, rows, keys = grads[0].shape
    feature = encodeds[0].shape[1]
    tile = 512
    grad_spec = pl.BlockSpec((1, tile, keys), lambda i, half: (half[0], i, 0))
    encoded_spec = pl.BlockSpec((keys, feature), lambda i, half: (0, 0))
    return pl.pallas_call(
        weight_kernel,
        grid_spec=pltpu.PrefetchScalarGridSpec(
            num_scalar_prefetch=1,
            grid=(rows // tile,),
            in_specs=[grad_spec, grad_spec, encoded_spec, encoded_spec],
            out_specs=pl.BlockSpec((tile, feature), lambda i, half: (i, 0)),
        ),
        out_shape=jax.ShapeDtypeStruct((rows, feature), BF16),
        cost_estimate=pl.CostEstimate(
            flops=4 * rows * feature * keys, bytes_accessed=8 << 20, transcendentals=0
        ),
        compiler_params=pltpu.CompilerParams(vmem_limit_bytes=60 << 20),
        name="weight_half",
    )(half, *grads, *encodeds)


def locate(block_ids, block_home):
    hits = block_ids[..., None] == jnp.arange(block_home.shape[0], dtype=jnp.int32)
    return jnp.sum(jnp.where(hits, block_home, 0), axis=-1)


def all_to_all(block, axis, groups=None):
    return lax.all_to_all(
        block, axis, split_axis=0, concat_axis=0, tiled=True, axis_index_groups=groups
    )


def summed(copies):
    return copies.astype(F32).sum(axis=0)


def local(
    hidden,
    database,
    block_home,
    neighbours,
    neighbour_counts,
    encoder_gain,
    encoder_projection,
    encoder_output,
    cross_gain,
    cross_query,
    cross_keyvalue,
    cross_output,
    cotangent,
):
    token_count, _ = hidden.shape
    _, length, feature = database.shape[1:]
    seq = lax.axis_size("seq")
    dp = lax.axis_size("dp")
    requests = neighbours.size
    tail = SPAN - 1

    tiles = feature // HEAD
    where = locate(neighbours.reshape(-1), block_home)
    notes = jnp.broadcast_to(jnp.pad(where, (0, HEAD - requests)), (length // seq, HEAD))
    slices, tails = spread(database[0], notes.astype(BF16), hidden, cotangent, seq)
    late = lax.ppermute(tails, "seq", [(i, i - 1) for i in range(1, seq)])
    late_hidden, late_cotangent = late[0, :tail], late[1, :tail]
    table = all_to_all(slices, "seq")
    readers_where = table[:, -1, 0, :requests].astype(jnp.int32)

    own_hidden = jnp.concatenate([hidden[tail:], late_hidden], axis=0)
    own_cotangent = jnp.concatenate([cotangent[tail:], late_cotangent], axis=0)
    normed = rms_norm(own_hidden, cross_gain).astype(BF16)
    queries = dot(normed, cross_query, NN).astype(BF16)
    grads = dot(own_cotangent, cross_output, NT).astype(BF16)

    chunks = 2
    encoded, grad_rows, attended = [], [], []
    picked = pick(readers_where, table, tiles, chunks)
    for part in range(chunks):
        pieces = all_to_all(picked[part], "seq")
        out = span_step(
            part,
            neighbour_counts,
            pieces,
            encoder_gain,
            encoder_projection,
            encoder_output,
            cross_keyvalue,
            queries,
            grads,
        )
        encoded.append(out[0])
        grad_rows.append(out[1])
        attended.append(out[2])

    core = lax.axis_index("dp") % 2
    theirs = weight_half((1 - core).reshape(1), grad_rows, encoded)
    received = lax.ppermute(theirs, "dp", [(i, i ^ 1) for i in range(dp)])
    mine = weight_half(core.reshape(1), grad_rows, encoded)
    pair = (mine.astype(F32) + received.astype(F32)).astype(BF16)

    half = [
        [d * seq + s for d in range(c, dp, 2) for s in range(seq)] for c in range(2)
    ]
    sent = all_to_all(pair.reshape(dp // 2 * seq, -1, feature), ("dp", "seq"), half)
    piece = summed(sent).astype(BF16)
    keyvalue_grad = all_to_all(jnp.broadcast_to(piece, (dp, *piece.shape)), "dp")
    keyvalue_grad = keyvalue_grad.reshape(-1, feature).astype(F32)

    cross = dot(jnp.concatenate(attended, axis=0), cross_output, NN)
    rows = (own_hidden.astype(F32) + cross).astype(BF16)
    forth = [(i, i + 1) for i in range(seq - 1)]
    returned = lax.ppermute(rows[token_count - tail :], "seq", forth)
    first = jnp.where(lax.axis_index("seq") == 0, hidden[:tail], returned)
    output = jnp.concatenate([first, rows[: token_count - tail]], axis=0)
    return (output, keyvalue_grad)


def solution(mesh):
    placed = (
        P(("dp", "seq"), None),
        P("dp", "seq", None, None),
        P(),
        P(("dp", "seq"), None),
        P(("dp", "seq")),
        P(),
        P(),
        P(),
        P(),
        P(),
        P(),
        P(),
        P(("dp", "seq"), None),
    )
    return jax.shard_map(
        local,
        mesh=mesh,
        in_specs=placed,
        out_specs=(P(("dp", "seq"), None), P("seq", None)),
        check_vma=False,
    )
```

```python
import functools

import jax
import jax.numpy as jnp
from jax import lax
from jax.experimental import pallas as pl
from jax.experimental.pallas import tpu as pltpu
from jax.sharding import PartitionSpec as P


HEAD = 128
K = 2
SPAN = 64
EPSILON = 1e-06
BF16 = jnp.bfloat16
F32 = jnp.float32
VMEM = pltpu.VMEM
NN = (((1,), (0,)), ((), ()))
NT = (((1,), (1,)), ((), ()))
TN = (((0,), (0,)), ((), ()))


def dot(a, b, dims):
    return lax.dot_general(a, b, dims, preferred_element_type=F32)


def rms_norm(values, norm_gain):
    widened = values.astype(F32)
    return (
        widened
        * lax.rsqrt(jnp.mean(widened * widened, axis=-1, keepdims=True) + EPSILON)
        * norm_gain
    )


def spread_kernel(home_ref, neighbours_ref, blocks_hbm, hidden_ref, cotangent_ref, slices_ref, tails_ref, blocks_ref, sems):
    blocks, length, feature = blocks_ref.shape
    devices, units, rows, _ = slices_ref.shape
    tiles = feature // HEAD
    parts = sems.shape[0]
    size = length // parts

    def load(part):
        part_rows = pl.ds(part * size, size)
        return pltpu.make_async_copy(
            blocks_hbm.at[:, part_rows], blocks_ref.at[:, part_rows], sems.at[part]
        )

    for part in range(parts):
        load(part).start()
    lane = lax.broadcasted_iota(jnp.int32, (rows, HEAD), 1)
    notes = jnp.zeros((rows, HEAD), jnp.int32)
    spans, each = neighbours_ref.shape
    for u in range(spans):
        for n in range(each):
            notes = jnp.where(lane == u * each + n, home_ref[neighbours_ref[u, n]], notes)
    notes = notes.astype(F32).astype(BF16)
    tails_ref[0] = hidden_ref[...]
    tails_ref[1] = cotangent_ref[...]
    for d in range(devices):
        if d % (devices // parts) == 0:
            load(d // (devices // parts)).wait()
        for b in range(blocks):
            for k in range(tiles):
                slices_ref[d, b * tiles + k] = blocks_ref[
                    b, d * rows : (d + 1) * rows, k * HEAD : (k + 1) * HEAD
                ]
        slices_ref[d, units - 1] = notes


def spread(block_home, neighbours, database, hidden, cotangent, devices):
    blocks, length, feature = database.shape
    width = hidden.shape[1]
    units = blocks * (feature // HEAD) + 1
    rows = length // devices
    smem = pl.BlockSpec(memory_space=pltpu.SMEM)
    first = pl.BlockSpec((SPAN, width), lambda i: (0, 0))
    whole = pl.BlockSpec(memory_space=VMEM)
    return pl.pallas_call(
        spread_kernel,
        grid=(1,),
        out_shape=(
            jax.ShapeDtypeStruct((devices, units, rows, HEAD), BF16),
            jax.ShapeDtypeStruct((2, SPAN, width), BF16),
        ),
        in_specs=[smem, smem, pl.BlockSpec(memory_space=pltpu.HBM), first, first],
        out_specs=(whole, whole),
        scratch_shapes=[VMEM(database.shape, BF16), pltpu.SemaphoreType.DMA((4,))],
        cost_estimate=pl.CostEstimate(flops=1 << 20, bytes_accessed=6 << 20, transcendentals=0),
        compiler_params=pltpu.CompilerParams(vmem_limit_bytes=60 << 20),
        name="spread",
    )(block_home, neighbours, database, hidden, cotangent)


def pick_kernel(tiles, where_ref, table_ref, *outs):
    blocks = table_ref.shape[1] // tiles

    @pl.loop(0, outs[0].shape[0])
    def _(r):
        first = 0
        for out in outs:
            for i in range(out.shape[1] // tiles):
                where = where_ref[r, first + i]
                start = (where % blocks) * tiles
                out[r, i * tiles : (i + 1) * tiles] = table_ref[
                    where // blocks, pl.ds(start, tiles)
                ]
            first += out.shape[1] // tiles


def pick(where, table, tiles, chunks):
    readers, requests = where.shape
    rows, width = table.shape[2:]
    shape = jax.ShapeDtypeStruct((readers, requests // chunks * tiles, rows, width), BF16)
    whole = pl.BlockSpec(memory_space=VMEM)
    return pl.pallas_call(
        functools.partial(pick_kernel, tiles),
        out_shape=(shape,) * chunks,
        in_specs=[pl.BlockSpec(memory_space=pltpu.SMEM), whole],
        out_specs=(whole,) * chunks,
        compiler_params=pltpu.CompilerParams(vmem_limit_bytes=60 << 20),
        name="pick",
    )(where, table)


def span_kernel(
    first_span,
    counts_ref,
    pieces_ref,
    gain_ref,
    projection_hbm,
    output_hbm,
    keyvalue_hbm,
    queries_ref,
    grads_ref,
    encoded_ref,
    grad_ref,
    attended_ref,
    projection_ref,
    output_ref,
    keyvalue_ref,
    plain_ref,
    normed_ref,
    qkv_ref,
    mixed_ref,
    kv_ref,
    encoder_scores_ref,
    encoder_weights_ref,
    scores_ref,
    changes_ref,
    chances_ref,
    grad_scores_ref,
    sems,
):
    slices, _, rows, _ = pieces_ref.shape
    length = slices * rows
    total, feature = encoded_ref.shape
    width = queries_ref.shape[1]
    blocks = total // length
    tiles = feature // HEAD
    heads = width // HEAD
    spans = blocks // K
    keys = K * length
    scale = HEAD ** (-0.5)
    chunk = 2 * width // (slices * 8)
    tile = 1024
    narrow = range(0, 3 * feature, tile)
    wide = range(0, 2 * width, tile)

    def load(j):
        columns = pl.ds(narrow[j], min(tile, 3 * feature - narrow[j]))
        return pltpu.make_async_copy(
            projection_hbm.at[:, columns], projection_ref.at[:, columns], sems.at[j]
        )

    def wide_load(j):
        columns = pl.ds(wide[j], tile)
        return pltpu.make_async_copy(
            keyvalue_hbm.at[columns], keyvalue_ref.at[columns], sems.at[len(narrow) + 1 + j]
        )

    output_load = pltpu.make_async_copy(output_hbm, output_ref, sems.at[len(narrow)])
    load(0).start()
    gain = gain_ref[...].reshape(1, feature)
    for b in range(blocks):
        block_rows = slice(b * length, (b + 1) * length)
        for k in range(tiles):
            plain_ref[block_rows, k * HEAD : (k + 1) * HEAD] = (
                pieces_ref[:, b * tiles + k].astype(F32).reshape(length, HEAD)
            )
        normed_ref[block_rows] = rms_norm(plain_ref[block_rows], gain).astype(BF16)

    for j in range(1, len(narrow)):
        load(j).start()
    for j in range(len(narrow)):
        load(j).wait()
        if j == 0:
            output_load.start()
        if j == 1:
            for i in range(len(wide)):
                wide_load(i).start()
        columns = slice(narrow[j], min(narrow[j] + tile, 3 * feature))
        qkv_ref[:, columns] = dot(normed_ref[...], projection_ref[:, columns], NN).astype(BF16)

    together = 2
    ones = jnp.ones((length, HEAD), BF16)

    @pl.loop(0, blocks // together)
    def _(step):
        pairs = [(b, h) for b in range(together) for h in range(tiles)]

        def part(which, b, h):
            start = pl.multiple_of((step * together + b) * length, length)
            return qkv_ref[pl.ds(start, length), pl.ds(which * feature + h * HEAD, HEAD)]

        for i, (b, h) in enumerate(pairs):
            encoder_scores_ref[i] = dot(part(0, b, h), part(1, b, h), NT) * scale
        tops = [jnp.max(encoder_scores_ref[i], axis=-1, keepdims=True) for i in range(len(pairs))]
        for i, top in enumerate(tops):
            encoder_weights_ref[i] = jnp.exp(encoder_scores_ref[i] - top).astype(BF16)
        for i, (b, h) in enumerate(pairs):
            value = jnp.concatenate([part(2, b, h), ones], axis=-1)
            summed_up = dot(encoder_weights_ref[i], value, NN)
            start = pl.multiple_of((step * together + b) * length, length)
            mixed_ref[pl.ds(start, length), h * HEAD : (h + 1) * HEAD] = (
                summed_up[:, :HEAD] / summed_up[:, HEAD:]
            ).astype(BF16)

    output_load.wait()
    for start in range(0, feature, 256):
        columns = slice(start, min(start + 256, feature))
        encoded_ref[:, columns] = (
            plain_ref[:, columns] + dot(mixed_ref[...], output_ref[:, columns], NN)
        ).astype(BF16)

    for j in range(len(wide)):
        wide_load(j).wait()
        columns = slice(wide[j], wide[j] + tile)
        kv_ref[:, columns] = dot(encoded_ref[...], keyvalue_ref[columns, :], NT).astype(BF16)

    key_block = lax.broadcasted_iota(jnp.int32, (1, keys), 1) // length

    @pl.loop(0, spans)
    def _(u):
        valid = key_block < counts_ref[first_span + u]
        query_rows = pl.ds(pl.multiple_of(u * SPAN, SPAN), SPAN)
        key_rows = pl.ds(pl.multiple_of(u * keys, keys), keys)

        def columns(h):
            return slice(h * HEAD, (h + 1) * HEAD)

        for h in range(heads):
            key = kv_ref[key_rows, columns(h)]
            value = kv_ref[key_rows, columns(heads + h)]
            scores = dot(queries_ref[query_rows, columns(h)], key, NT) * scale
            scores_ref[h] = jnp.where(valid, scores, -1e30)
            changes_ref[h] = dot(grads_ref[query_rows, columns(h)], value, NT)
        tops = [jnp.max(scores_ref[h], axis=-1, keepdims=True) for h in range(heads)]
        for h in range(heads):
            scores_ref[h] = jnp.exp(scores_ref[h] - tops[h])
        sums = [jnp.sum(scores_ref[h], axis=-1, keepdims=True) for h in range(heads)]
        for h in range(heads):
            chances = scores_ref[h] * (1.0 / sums[h])
            scores_ref[h] = chances
            chances_ref[h] = chances.astype(BF16)
        inners = [
            jnp.sum(scores_ref[h] * changes_ref[h], axis=-1, keepdims=True) for h in range(heads)
        ]
        for h in range(heads):
            grad_scores_ref[h] = (scores_ref[h] * (changes_ref[h] - inners[h])).astype(BF16)
        for h in range(heads):
            value = kv_ref[key_rows, columns(heads + h)]
            query = queries_ref[query_rows, columns(h)]
            grad = grads_ref[query_rows, columns(h)]
            attended_ref[query_rows, columns(h)] = dot(chances_ref[h], value, NN).astype(BF16)
            for part, piece in enumerate(
                (
                    dot(query, grad_scores_ref[h], TN) * scale,
                    dot(grad, chances_ref[h], TN),
                )
            ):
                for j in range(HEAD // 8):
                    row = part * width + h * HEAD + j * 8
                    seq, inside = divmod(row, 8 * chunk)
                    dp, offset = divmod(inside, chunk)
                    base = ((dp // 2) * slices + seq) * chunk + offset
                    grad_ref[dp % 2, base : base + 8, key_rows] = piece[j * 8 : j * 8 + 8].astype(
                        BF16
                    )


def span_step(part, counts, pieces, gain, projection, output, keyvalue, queries, grads):
    width = queries.shape[1]
    feature = keyvalue.shape[1]
    slices, units, rows, _ = pieces.shape
    tiles = feature // HEAD
    length = slices * rows
    blocks = units // tiles
    total = blocks * length
    spans = blocks // K
    keys = K * length
    heads = width // HEAD
    whole = pl.BlockSpec(memory_space=VMEM)
    hbm = pl.BlockSpec(memory_space=pltpu.HBM)
    own = pl.BlockSpec((spans * SPAN, width), lambda i: (part, 0))
    return pl.pallas_call(
        functools.partial(span_kernel, part * spans),
        grid=(1,),
        out_shape=(
            jax.ShapeDtypeStruct((total, feature), BF16),
            jax.ShapeDtypeStruct((2, width, total), BF16),
            jax.ShapeDtypeStruct((spans * SPAN, width), BF16),
        ),
        in_specs=[
            pl.BlockSpec(memory_space=pltpu.SMEM),
            whole,
            whole,
            hbm,
            hbm,
            hbm,
            own,
            own,
        ],
        out_specs=(whole, whole, whole),
        scratch_shapes=[
            VMEM(projection.shape, BF16),
            VMEM(output.shape, BF16),
            VMEM(keyvalue.shape, BF16),
            VMEM((total, feature), F32),
            VMEM((total, feature), BF16),
            VMEM((total, 3 * feature), BF16),
            VMEM((total, feature), BF16),
            VMEM((total, 2 * width), BF16),
            VMEM((2 * tiles, length, length), F32),
            VMEM((2 * tiles, length, length), BF16),
            VMEM((heads, SPAN, keys), F32),
            VMEM((heads, SPAN, keys), F32),
            VMEM((heads, SPAN, keys), BF16),
            VMEM((heads, SPAN, keys), BF16),
            pltpu.SemaphoreType.DMA((pl.cdiv(3 * feature, 1024) + 1 + 2 * width // 1024,)),
        ],
        cost_estimate=pl.CostEstimate(
            flops=total * feature * (8 * feature + 4 * width),
            bytes_accessed=20 << 20,
            transcendentals=1 << 20,
        ),
        compiler_params=pltpu.CompilerParams(vmem_limit_bytes=(60, 54)[part] << 20),
        name="spans",
    )(counts, pieces, gain, projection, output, keyvalue, queries, grads)


def weight_kernel(half_ref, grad_a, grad_b, encoded_a, encoded_b, out_ref):
    out_ref[...] = (
        dot(grad_a[0], encoded_a[...], NN) + dot(grad_b[0], encoded_b[...], NN)
    ).astype(BF16)


def weight_half(half, grads, encodeds):
    _, rows, keys = grads[0].shape
    feature = encodeds[0].shape[1]
    tile = 512
    grad_spec = pl.BlockSpec((1, tile, keys), lambda i, half: (half[0], i, 0))
    encoded_spec = pl.BlockSpec((keys, feature), lambda i, half: (0, 0))
    return pl.pallas_call(
        weight_kernel,
        grid_spec=pltpu.PrefetchScalarGridSpec(
            num_scalar_prefetch=1,
            grid=(rows // tile,),
            in_specs=[grad_spec, grad_spec, encoded_spec, encoded_spec],
            out_specs=pl.BlockSpec((tile, feature), lambda i, half: (i, 0)),
        ),
        out_shape=jax.ShapeDtypeStruct((rows, feature), BF16),
        cost_estimate=pl.CostEstimate(
            flops=4 * rows * feature * keys, bytes_accessed=8 << 20, transcendentals=0
        ),
        compiler_params=pltpu.CompilerParams(vmem_limit_bytes=24 << 20),
        name="weight_half",
    )(half, *grads, *encodeds)


def all_to_all(block, axis, groups=None):
    return lax.all_to_all(
        block, axis, split_axis=0, concat_axis=0, tiled=True, axis_index_groups=groups
    )


def summed(copies):
    return copies.astype(F32).sum(axis=0)


def local(
    hidden,
    database,
    block_home,
    neighbours,
    neighbour_counts,
    encoder_gain,
    encoder_projection,
    encoder_output,
    cross_gain,
    cross_query,
    cross_keyvalue,
    cross_output,
    cotangent,
):
    token_count, _ = hidden.shape
    _, _, feature = database.shape[1:]
    seq = lax.axis_size("seq")
    dp = lax.axis_size("dp")
    requests = neighbours.size
    tail = SPAN - 1

    tiles = feature // HEAD
    slices, tails = spread(block_home, neighbours, database[0], hidden, cotangent, seq)
    late = lax.ppermute(tails, "seq", [(i, i - 1) for i in range(1, seq)])
    late_hidden, late_cotangent = late[0, :tail], late[1, :tail]
    table = all_to_all(slices, "seq")
    readers_where = table[:, -1, 0, :requests].astype(jnp.int32)

    own_hidden = jnp.concatenate([hidden[tail:], late_hidden], axis=0)
    own_cotangent = jnp.concatenate([cotangent[tail:], late_cotangent], axis=0)
    normed = rms_norm(own_hidden, cross_gain).astype(BF16)
    queries = dot(normed, cross_query, NN).astype(BF16)
    grads = dot(own_cotangent, cross_output, NT).astype(BF16)

    chunks = 2
    encoded, grad_rows, attended = [], [], []
    picked = pick(readers_where, table, tiles, chunks)
    for part in range(chunks):
        pieces = all_to_all(picked[part], "seq")
        out = span_step(
            part,
            neighbour_counts,
            pieces,
            encoder_gain,
            encoder_projection,
            encoder_output,
            cross_keyvalue,
            queries,
            grads,
        )
        encoded.append(out[0])
        grad_rows.append(out[1])
        attended.append(out[2])

    core = lax.axis_index("dp") % 2
    theirs = weight_half((1 - core).reshape(1), grad_rows, encoded)
    received = lax.ppermute(theirs, "dp", [(i, i ^ 1) for i in range(dp)])
    mine = weight_half(core.reshape(1), grad_rows, encoded)
    pair = (mine.astype(F32) + received.astype(F32)).astype(BF16)

    half = [
        [d * seq + s for d in range(c, dp, 2) for s in range(seq)] for c in range(2)
    ]
    sent = all_to_all(pair.reshape(dp // 2 * seq, -1, feature), ("dp", "seq"), half)
    piece = summed(sent).astype(BF16)
    keyvalue_grad = all_to_all(jnp.broadcast_to(piece, (dp, *piece.shape)), "dp")
    keyvalue_grad = keyvalue_grad.reshape(-1, feature).astype(F32)

    cross = dot(jnp.concatenate(attended, axis=0), cross_output, NN)
    rows = (own_hidden.astype(F32) + cross).astype(BF16)
    forth = [(i, i + 1) for i in range(seq - 1)]
    returned = lax.ppermute(rows[token_count - tail :], "seq", forth)
    first = jnp.where(lax.axis_index("seq") == 0, hidden[:tail], returned)
    output = jnp.concatenate([first, rows[: token_count - tail]], axis=0)
    return (output, keyvalue_grad)


def solution(mesh):
    placed = (
        P(("dp", "seq"), None),
        P("dp", "seq", None, None),
        P(),
        P(("dp", "seq"), None),
        P(("dp", "seq")),
        P(),
        P(),
        P(),
        P(),
        P(),
        P(),
        P(),
        P(("dp", "seq"), None),
    )
    return jax.shard_map(
        local,
        mesh=mesh,
        in_specs=placed,
        out_specs=(P(("dp", "seq"), None), P("seq", None)),
        check_vma=False,
    )
```

```python
import functools

import jax
import jax.numpy as jnp
from jax import lax
from jax.experimental import pallas as pl
from jax.experimental.pallas import tpu as pltpu
from jax.sharding import PartitionSpec as P


HEAD = 128
K = 2
SPAN = 64
EPSILON = 1e-06
BF16 = jnp.bfloat16
F32 = jnp.float32
VMEM = pltpu.VMEM
NN = (((1,), (0,)), ((), ()))
NT = (((1,), (1,)), ((), ()))
TN = (((0,), (0,)), ((), ()))


def dot(a, b, dims):
    return lax.dot_general(a, b, dims, preferred_element_type=F32)


def rms_norm(values, norm_gain):
    widened = values.astype(F32)
    return (
        widened
        * lax.rsqrt(jnp.mean(widened * widened, axis=-1, keepdims=True) + EPSILON)
        * norm_gain
    )


def spread_kernel(
    home_ref,
    neighbours_ref,
    blocks_hbm,
    hidden_ref,
    cotangent_ref,
    slices_hbm,
    tails_ref,
    blocks_ref,
    slices_ref,
    sems,
    out_sems,
):
    blocks, length, feature = blocks_ref.shape
    devices, units, rows, _ = slices_ref.shape
    tiles = feature // HEAD
    parts = sems.shape[0]
    size = length // parts

    def load(part):
        part_rows = pl.ds(part * size, size)
        return pltpu.make_async_copy(
            blocks_hbm.at[:, part_rows], blocks_ref.at[:, part_rows], sems.at[part]
        )

    def store(part):
        several = pl.ds(part * (devices // parts), devices // parts)
        return pltpu.make_async_copy(
            slices_ref.at[several], slices_hbm.at[several], out_sems.at[part]
        )

    for part in range(parts):
        load(part).start()
    lane = lax.broadcasted_iota(jnp.int32, (rows, HEAD), 1)
    notes = jnp.zeros((rows, HEAD), jnp.int32)
    spans, each = neighbours_ref.shape
    for u in range(spans):
        for n in range(each):
            notes = jnp.where(lane == u * each + n, home_ref[neighbours_ref[u, n]], notes)
    notes = notes.astype(F32).astype(BF16)
    tails_ref[0] = hidden_ref[...]
    tails_ref[1] = cotangent_ref[...]
    for d in range(devices):
        if d % (devices // parts) == 0:
            load(d // (devices // parts)).wait()
        for b in range(blocks):
            for k in range(tiles):
                slices_ref[d, b * tiles + k] = blocks_ref[
                    b, d * rows : (d + 1) * rows, k * HEAD : (k + 1) * HEAD
                ]
        slices_ref[d, units - 1] = notes
        if (d + 1) % (devices // parts) == 0:
            store(d // (devices // parts)).start()
    for part in range(parts):
        store(part).wait()


def spread(block_home, neighbours, database, hidden, cotangent, devices):
    blocks, length, feature = database.shape
    width = hidden.shape[1]
    units = blocks * (feature // HEAD) + 1
    rows = length // devices
    smem = pl.BlockSpec(memory_space=pltpu.SMEM)
    first = pl.BlockSpec((SPAN, width), lambda i: (0, 0))
    whole = pl.BlockSpec(memory_space=VMEM)
    return pl.pallas_call(
        spread_kernel,
        grid=(1,),
        out_shape=(
            jax.ShapeDtypeStruct((devices, units, rows, HEAD), BF16),
            jax.ShapeDtypeStruct((2, SPAN, width), BF16),
        ),
        in_specs=[smem, smem, pl.BlockSpec(memory_space=pltpu.HBM), first, first],
        out_specs=(pl.BlockSpec(memory_space=pltpu.HBM), whole),
        scratch_shapes=[
            VMEM(database.shape, BF16),
            VMEM((devices, units, rows, HEAD), BF16),
            pltpu.SemaphoreType.DMA((4,)),
            pltpu.SemaphoreType.DMA((4,)),
        ],
        cost_estimate=pl.CostEstimate(flops=1 << 20, bytes_accessed=6 << 20, transcendentals=0),
        compiler_params=pltpu.CompilerParams(vmem_limit_bytes=60 << 20),
        name="spread",
    )(block_home, neighbours, database, hidden, cotangent)


def pick_kernel(tiles, where_ref, table_ref, out_ref):
    blocks = table_ref.shape[1] // tiles

    @pl.loop(0, out_ref.shape[0])
    def _(r):
        for i in range(out_ref.shape[1] // tiles):
            where = where_ref[r, i]
            start = (where % blocks) * tiles
            out_ref[r, i * tiles : (i + 1) * tiles] = table_ref[
                where // blocks, pl.ds(start, tiles)
            ]


def pick(where, table, tiles):
    readers, requests = where.shape
    rows, width = table.shape[2:]
    whole = pl.BlockSpec(memory_space=VMEM)
    return pl.pallas_call(
        functools.partial(pick_kernel, tiles),
        out_shape=jax.ShapeDtypeStruct((readers, requests * tiles, rows, width), BF16),
        in_specs=[pl.BlockSpec(memory_space=pltpu.SMEM), whole],
        out_specs=whole,
        compiler_params=pltpu.CompilerParams(vmem_limit_bytes=60 << 20),
        name="pick",
    )(where, table)


def span_kernel(
    counts_ref,
    theirs_ref,
    pieces_ref,
    gain_ref,
    projection_hbm,
    output_hbm,
    keyvalue_hbm,
    queries_ref,
    grads_ref,
    encoded_hbm,
    own_hbm,
    product_hbm,
    attended_ref,
    projection_ref,
    output_ref,
    keyvalue_ref,
    plain_ref,
    normed_ref,
    qkv_ref,
    mixed_ref,
    kv_ref,
    encoder_scores_ref,
    encoder_weights_ref,
    scores_ref,
    changes_ref,
    chances_ref,
    grad_scores_ref,
    encoded_ref,
    grad_ref,
    product_ref,
    sems,
    out_sems,
):
    slices, _, rows, _ = pieces_ref.shape
    length = slices * rows
    total, feature = encoded_ref.shape
    width = queries_ref.shape[1]
    blocks = total // length
    tiles = feature // HEAD
    heads = width // HEAD
    spans = blocks // K
    keys = K * length
    scale = HEAD ** (-0.5)
    chunk = 2 * width // (slices * 8)
    tile = 1024
    narrow = range(0, 3 * feature, tile)
    wide = range(0, 2 * width, tile)

    def load(j):
        columns = pl.ds(narrow[j], min(tile, 3 * feature - narrow[j]))
        return pltpu.make_async_copy(
            projection_hbm.at[:, columns], projection_ref.at[:, columns], sems.at[j]
        )

    def wide_load(j):
        columns = pl.ds(wide[j], tile)
        return pltpu.make_async_copy(
            keyvalue_hbm.at[columns], keyvalue_ref.at[columns], sems.at[len(narrow) + 1 + j]
        )

    output_load = pltpu.make_async_copy(output_hbm, output_ref, sems.at[len(narrow)])
    load(0).start()
    gain = gain_ref[...].reshape(1, feature)
    for b in range(blocks):
        block_rows = slice(b * length, (b + 1) * length)
        for k in range(tiles):
            plain_ref[block_rows, k * HEAD : (k + 1) * HEAD] = (
                pieces_ref[:, b * tiles + k].astype(F32).reshape(length, HEAD)
            )
        normed_ref[block_rows] = rms_norm(plain_ref[block_rows], gain).astype(BF16)

    for j in range(1, len(narrow)):
        load(j).start()
    for j in range(len(narrow)):
        load(j).wait()
        if j == 0:
            output_load.start()
        if j == 1:
            for i in range(len(wide)):
                wide_load(i).start()
        columns = slice(narrow[j], min(narrow[j] + tile, 3 * feature))
        qkv_ref[:, columns] = dot(normed_ref[...], projection_ref[:, columns], NN).astype(BF16)

    together = 2
    ones = jnp.ones((length, HEAD), BF16)

    @pl.loop(0, blocks // together)
    def _(step):
        pairs = [(b, h) for b in range(together) for h in range(tiles)]

        def part(which, b, h):
            start = pl.multiple_of((step * together + b) * length, length)
            return qkv_ref[pl.ds(start, length), pl.ds(which * feature + h * HEAD, HEAD)]

        for i, (b, h) in enumerate(pairs):
            encoder_scores_ref[i] = dot(part(0, b, h), part(1, b, h), NT) * scale
        tops = [jnp.max(encoder_scores_ref[i], axis=-1, keepdims=True) for i in range(len(pairs))]
        for i, top in enumerate(tops):
            encoder_weights_ref[i] = jnp.exp(encoder_scores_ref[i] - top).astype(BF16)
        for i, (b, h) in enumerate(pairs):
            value = jnp.concatenate([part(2, b, h), ones], axis=-1)
            summed_up = dot(encoder_weights_ref[i], value, NN)
            start = pl.multiple_of((step * together + b) * length, length)
            mixed_ref[pl.ds(start, length), h * HEAD : (h + 1) * HEAD] = (
                summed_up[:, :HEAD] / summed_up[:, HEAD:]
            ).astype(BF16)

    output_load.wait()
    for start in range(0, feature, 256):
        columns = slice(start, min(start + 256, feature))
        encoded_ref[:, columns] = (
            plain_ref[:, columns] + dot(mixed_ref[...], output_ref[:, columns], NN)
        ).astype(BF16)

    stores = [pltpu.make_async_copy(encoded_ref, encoded_hbm, out_sems.at[0])]
    stores[0].start()
    for j in range(len(wide)):
        wide_load(j).wait()
        columns = slice(wide[j], wide[j] + tile)
        kv_ref[:, columns] = dot(encoded_ref[...], keyvalue_ref[columns, :], NT).astype(BF16)

    key_block = lax.broadcasted_iota(jnp.int32, (1, keys), 1) // length

    @pl.loop(0, spans)
    def _(u):
        valid = key_block < counts_ref[u]
        query_rows = pl.ds(pl.multiple_of(u * SPAN, SPAN), SPAN)
        key_rows = pl.ds(pl.multiple_of(u * keys, keys), keys)

        def columns(h):
            return slice(h * HEAD, (h + 1) * HEAD)

        for h in range(heads):
            key = kv_ref[key_rows, columns(h)]
            value = kv_ref[key_rows, columns(heads + h)]
            scores = dot(queries_ref[query_rows, columns(h)], key, NT) * scale
            scores_ref[h] = jnp.where(valid, scores, -1e30)
            changes_ref[h] = dot(grads_ref[query_rows, columns(h)], value, NT)
        tops = [jnp.max(scores_ref[h], axis=-1, keepdims=True) for h in range(heads)]
        for h in range(heads):
            scores_ref[h] = jnp.exp(scores_ref[h] - tops[h])
        sums = [jnp.sum(scores_ref[h], axis=-1, keepdims=True) for h in range(heads)]
        for h in range(heads):
            chances = scores_ref[h] * (1.0 / sums[h])
            scores_ref[h] = chances
            chances_ref[h] = chances.astype(BF16)
        inners = [
            jnp.sum(scores_ref[h] * changes_ref[h], axis=-1, keepdims=True) for h in range(heads)
        ]
        for h in range(heads):
            grad_scores_ref[h] = (scores_ref[h] * (changes_ref[h] - inners[h])).astype(BF16)
        for h in range(heads):
            value = kv_ref[key_rows, columns(heads + h)]
            query = queries_ref[query_rows, columns(h)]
            grad = grads_ref[query_rows, columns(h)]
            attended_ref[query_rows, columns(h)] = dot(chances_ref[h], value, NN).astype(BF16)
            for part, piece in enumerate(
                (
                    dot(query, grad_scores_ref[h], TN) * scale,
                    dot(grad, chances_ref[h], TN),
                )
            ):
                for j in range(HEAD // 8):
                    row = part * width + h * HEAD + j * 8
                    seq, inside = divmod(row, 8 * chunk)
                    dp, offset = divmod(inside, chunk)
                    base = ((dp // 2) * slices + seq) * chunk + offset
                    grad_ref[dp % 2, base : base + 8, key_rows] = piece[j * 8 : j * 8 + 8].astype(
                        BF16
                    )

    theirs = theirs_ref[0]
    stores.append(pltpu.make_async_copy(grad_ref.at[1 - theirs], own_hbm, out_sems.at[1]))
    stores[1].start()
    for i in range(width // 512):
        part = slice(i * 512, (i + 1) * 512)
        product_ref[part] = dot(grad_ref[theirs, part], encoded_ref[...], NN).astype(BF16)
        stores.append(
            pltpu.make_async_copy(
                product_ref.at[part], product_hbm.at[part], out_sems.at[2 + i]
            )
        )
        stores[-1].start()
    for store in stores:
        store.wait()


def span_step(counts, theirs, pieces, gain, projection, output, keyvalue, queries, grads):
    width = queries.shape[1]
    feature = keyvalue.shape[1]
    slices, units, rows, _ = pieces.shape
    tiles = feature // HEAD
    length = slices * rows
    blocks = units // tiles
    total = blocks * length
    spans = blocks // K
    keys = K * length
    heads = width // HEAD
    whole = pl.BlockSpec(memory_space=VMEM)
    hbm = pl.BlockSpec(memory_space=pltpu.HBM)
    return pl.pallas_call(
        span_kernel,
        out_shape=(
            jax.ShapeDtypeStruct((total, feature), BF16),
            jax.ShapeDtypeStruct((width, total), BF16),
            jax.ShapeDtypeStruct((width, feature), BF16),
            jax.ShapeDtypeStruct((spans * SPAN, width), BF16),
        ),
        in_specs=[
            pl.BlockSpec(memory_space=pltpu.SMEM),
            pl.BlockSpec(memory_space=pltpu.SMEM),
            whole,
            whole,
            hbm,
            hbm,
            hbm,
            whole,
            whole,
        ],
        out_specs=(hbm, hbm, hbm, whole),
        scratch_shapes=[
            VMEM(projection.shape, BF16),
            VMEM(output.shape, BF16),
            VMEM(keyvalue.shape, BF16),
            VMEM((total, feature), F32),
            VMEM((total, feature), BF16),
            VMEM((total, 3 * feature), BF16),
            VMEM((total, feature), BF16),
            VMEM((total, 2 * width), BF16),
            VMEM((2 * tiles, length, length), F32),
            VMEM((2 * tiles, length, length), BF16),
            VMEM((heads, SPAN, keys), F32),
            VMEM((heads, SPAN, keys), F32),
            VMEM((heads, SPAN, keys), BF16),
            VMEM((heads, SPAN, keys), BF16),
            VMEM((total, feature), BF16),
            VMEM((2, width, total), BF16),
            VMEM((width, feature), BF16),
            pltpu.SemaphoreType.DMA((pl.cdiv(3 * feature, 1024) + 1 + 2 * width // 1024,)),
            pltpu.SemaphoreType.DMA((2 + width // 512,)),
        ],
        cost_estimate=pl.CostEstimate(
            flops=total * feature * (8 * feature + 6 * width),
            bytes_accessed=20 << 20,
            transcendentals=1 << 20,
        ),
        compiler_params=pltpu.CompilerParams(vmem_limit_bytes=58 << 20),
        name="spans",
    )(counts, theirs, pieces, gain, projection, output, keyvalue, queries, grads)


def weight_kernel(grad_ref, encoded_ref, out_ref):
    out_ref[...] = dot(grad_ref[...], encoded_ref[...], NN).astype(BF16)


def weight_half(grad, encoded):
    rows, keys = grad.shape
    feature = encoded.shape[1]
    tile = 512
    return pl.pallas_call(
        weight_kernel,
        grid=(rows // tile,),
        in_specs=[
            pl.BlockSpec((tile, keys), lambda i: (i, 0)),
            pl.BlockSpec((keys, feature), lambda i: (0, 0)),
        ],
        out_specs=pl.BlockSpec((tile, feature), lambda i: (i, 0)),
        out_shape=jax.ShapeDtypeStruct((rows, feature), BF16),
        cost_estimate=pl.CostEstimate(
            flops=2 * rows * feature * keys, bytes_accessed=8 << 20, transcendentals=0
        ),
        compiler_params=pltpu.CompilerParams(vmem_limit_bytes=24 << 20),
        name="weight_half",
    )(grad, encoded)


def total_kernel(terms_ref, out_ref):
    total = jnp.sum(terms_ref[...].astype(F32), axis=0).astype(BF16)
    for i in range(out_ref.shape[0]):
        out_ref[i] = total


def total_copies(terms, copies):
    whole = pl.BlockSpec(memory_space=VMEM)
    return pl.pallas_call(
        total_kernel,
        out_shape=jax.ShapeDtypeStruct((copies, *terms.shape[1:]), BF16),
        in_specs=[whole],
        out_specs=whole,
        compiler_params=pltpu.CompilerParams(vmem_limit_bytes=16 << 20),
        name="total",
    )(terms)


def all_to_all(block, axis, groups=None):
    return lax.all_to_all(
        block, axis, split_axis=0, concat_axis=0, tiled=True, axis_index_groups=groups
    )


def local(
    hidden,
    database,
    block_home,
    neighbours,
    neighbour_counts,
    encoder_gain,
    encoder_projection,
    encoder_output,
    cross_gain,
    cross_query,
    cross_keyvalue,
    cross_output,
    cotangent,
):
    token_count, _ = hidden.shape
    _, _, feature = database.shape[1:]
    seq = lax.axis_size("seq")
    dp = lax.axis_size("dp")
    requests = neighbours.size
    tail = SPAN - 1

    tiles = feature // HEAD
    slices, tails = spread(block_home, neighbours, database[0], hidden, cotangent, seq)
    late = lax.ppermute(tails, "seq", [(i, i - 1) for i in range(1, seq)])
    late_hidden, late_cotangent = late[0, :tail], late[1, :tail]
    table = all_to_all(slices, "seq")
    readers_where = table[:, -1, 0, :requests].astype(jnp.int32)

    own_hidden = jnp.concatenate([hidden[tail:], late_hidden], axis=0)
    own_cotangent = jnp.concatenate([cotangent[tail:], late_cotangent], axis=0)
    normed = rms_norm(own_hidden, cross_gain).astype(BF16)
    queries = dot(normed, cross_query, NN).astype(BF16)
    grads = dot(own_cotangent, cross_output, NT).astype(BF16)

    picked = pick(readers_where, table, tiles)
    pieces = all_to_all(picked, "seq")
    core = lax.axis_index("dp") % 2
    encoded, own, theirs, attended = span_step(
        neighbour_counts,
        (1 - core).reshape(1),
        pieces,
        encoder_gain,
        encoder_projection,
        encoder_output,
        cross_keyvalue,
        queries,
        grads,
    )
    received = lax.ppermute(theirs, "dp", [(i, i ^ 1) for i in range(dp)])
    mine = weight_half(own, encoded)
    pair = (mine.astype(F32) + received.astype(F32)).astype(BF16)

    half = [
        [d * seq + s for d in range(c, dp, 2) for s in range(seq)] for c in range(2)
    ]
    sent = all_to_all(pair.reshape(dp // 2 * seq, -1, feature), ("dp", "seq"), half)
    keyvalue_grad = all_to_all(total_copies(sent, dp), "dp")
    keyvalue_grad = keyvalue_grad.reshape(-1, feature).astype(F32)

    cross = dot(attended, cross_output, NN)
    rows = (own_hidden.astype(F32) + cross).astype(BF16)
    forth = [(i, i + 1) for i in range(seq - 1)]
    returned = lax.ppermute(rows[token_count - tail :], "seq", forth)
    first = jnp.where(lax.axis_index("seq") == 0, hidden[:tail], returned)
    output = jnp.concatenate([first, rows[: token_count - tail]], axis=0)
    return (output, keyvalue_grad)


def solution(mesh):
    placed = (
        P(("dp", "seq"), None),
        P("dp", "seq", None, None),
        P(),
        P(("dp", "seq"), None),
        P(("dp", "seq")),
        P(),
        P(),
        P(),
        P(),
        P(),
        P(),
        P(),
        P(("dp", "seq"), None),
    )
    return jax.shard_map(
        local,
        mesh=mesh,
        in_specs=placed,
        out_specs=(P(("dp", "seq"), None), P("seq", None)),
        check_vma=False,
    )
```

```python
import functools

import jax
import jax.numpy as jnp
from jax import lax
from jax.experimental import pallas as pl
from jax.experimental.pallas import tpu as pltpu
from jax.sharding import PartitionSpec as P


HEAD = 128
K = 2
SPAN = 64
EPSILON = 1e-06
BF16 = jnp.bfloat16
F32 = jnp.float32
VMEM = pltpu.VMEM
NN = (((1,), (0,)), ((), ()))
NT = (((1,), (1,)), ((), ()))
TN = (((0,), (0,)), ((), ()))


def dot(a, b, dims):
    return lax.dot_general(a, b, dims, preferred_element_type=F32)


def rms_norm(values, norm_gain):
    widened = values.astype(F32)
    return (
        widened
        * lax.rsqrt(jnp.mean(widened * widened, axis=-1, keepdims=True) + EPSILON)
        * norm_gain
    )


def spread_kernel(
    home_ref,
    neighbours_ref,
    blocks_hbm,
    hidden_hbm,
    cotangent_hbm,
    slices_hbm,
    tails_hbm,
    blocks_ref,
    slices_ref,
    tails_ref,
    sems,
    out_sems,
    tail_sems,
):
    blocks, length, feature = blocks_ref.shape
    devices, units, rows, _ = slices_ref.shape
    tiles = feature // HEAD
    parts = sems.shape[0]
    size = length // parts

    def load(part):
        part_rows = pl.ds(part * size, size)
        return pltpu.make_async_copy(
            blocks_hbm.at[:, part_rows], blocks_ref.at[:, part_rows], sems.at[part]
        )

    def store(part):
        several = pl.ds(part * (devices // parts), devices // parts)
        return pltpu.make_async_copy(
            slices_ref.at[several], slices_hbm.at[several], out_sems.at[part]
        )

    span = tails_ref.shape[1]
    tail_loads = [
        pltpu.make_async_copy(rows_hbm.at[pl.ds(0, span)], tails_ref.at[i], tail_sems.at[i])
        for i, rows_hbm in enumerate((hidden_hbm, cotangent_hbm))
    ]
    tail_store = pltpu.make_async_copy(tails_ref, tails_hbm, tail_sems.at[2])
    for part in range(parts):
        load(part).start()
        if part == 0:
            for tail_load in tail_loads:
                tail_load.start()
    lane = lax.broadcasted_iota(jnp.int32, (rows, HEAD), 1)
    notes = jnp.zeros((rows, HEAD), jnp.int32)
    spans, each = neighbours_ref.shape
    for u in range(spans):
        for n in range(each):
            notes = jnp.where(lane == u * each + n, home_ref[neighbours_ref[u, n]], notes)
    notes = notes.astype(F32).astype(BF16)
    for d in range(devices):
        if d % (devices // parts) == 0:
            load(d // (devices // parts)).wait()
        for b in range(blocks):
            for k in range(tiles):
                slices_ref[d, b * tiles + k] = blocks_ref[
                    b, d * rows : (d + 1) * rows, k * HEAD : (k + 1) * HEAD
                ]
        slices_ref[d, units - 1] = notes
        if (d + 1) % (devices // parts) == 0:
            store(d // (devices // parts)).start()
            if d < devices // parts:
                for tail_load in tail_loads:
                    tail_load.wait()
                tail_store.start()
    for part in range(parts):
        store(part).wait()
    tail_store.wait()


def spread(block_home, neighbours, database, hidden, cotangent, devices):
    blocks, length, feature = database.shape
    width = hidden.shape[1]
    units = blocks * (feature // HEAD) + 1
    rows = length // devices
    smem = pl.BlockSpec(memory_space=pltpu.SMEM)
    hbm = pl.BlockSpec(memory_space=pltpu.HBM)
    return pl.pallas_call(
        spread_kernel,
        out_shape=(
            jax.ShapeDtypeStruct((devices, units, rows, HEAD), BF16),
            jax.ShapeDtypeStruct((2, SPAN, width), BF16),
        ),
        in_specs=[smem, smem, hbm, hbm, hbm],
        out_specs=(hbm, hbm),
        scratch_shapes=[
            VMEM(database.shape, BF16),
            VMEM((devices, units, rows, HEAD), BF16),
            VMEM((2, SPAN, width), BF16),
            pltpu.SemaphoreType.DMA((4,)),
            pltpu.SemaphoreType.DMA((4,)),
            pltpu.SemaphoreType.DMA((3,)),
        ],
        cost_estimate=pl.CostEstimate(flops=1 << 20, bytes_accessed=6 << 20, transcendentals=0),
        compiler_params=pltpu.CompilerParams(vmem_limit_bytes=60 << 20),
        name="spread",
    )(block_home, neighbours, database, hidden, cotangent)


def pick_kernel(tiles, where_ref, table_ref, out_hbm, out_ref, sems):
    blocks = table_ref.shape[1] // tiles
    parts = sems.shape[0]
    size = out_ref.shape[0] // parts

    def store(part):
        readers = pl.ds(part * size, size)
        return pltpu.make_async_copy(out_ref.at[readers], out_hbm.at[readers], sems.at[part])

    for part in range(parts):

        @pl.loop(part * size, (part + 1) * size)
        def _(r):
            for i in range(out_ref.shape[1] // tiles):
                where = where_ref[r, i]
                start = (where % blocks) * tiles
                out_ref[r, i * tiles : (i + 1) * tiles] = table_ref[
                    where // blocks, pl.ds(start, tiles)
                ]

        store(part).start()
    for part in range(parts):
        store(part).wait()


def pick(where, table, tiles):
    readers, requests = where.shape
    rows, width = table.shape[2:]
    shape = (readers, requests * tiles, rows, width)
    whole = pl.BlockSpec(memory_space=VMEM)
    return pl.pallas_call(
        functools.partial(pick_kernel, tiles),
        out_shape=jax.ShapeDtypeStruct(shape, BF16),
        in_specs=[pl.BlockSpec(memory_space=pltpu.SMEM), whole],
        out_specs=pl.BlockSpec(memory_space=pltpu.HBM),
        scratch_shapes=[VMEM(shape, BF16), pltpu.SemaphoreType.DMA((4,))],
        compiler_params=pltpu.CompilerParams(vmem_limit_bytes=60 << 20),
        name="pick",
    )(where, table)


def span_kernel(
    counts_ref,
    theirs_ref,
    pieces_hbm,
    gain_ref,
    projection_hbm,
    output_hbm,
    keyvalue_hbm,
    queries_hbm,
    grads_hbm,
    encoded_hbm,
    own_hbm,
    product_hbm,
    attended_ref,
    projection_ref,
    output_ref,
    keyvalue_ref,
    plain_ref,
    normed_ref,
    qkv_ref,
    mixed_ref,
    kv_ref,
    encoder_scores_ref,
    encoder_weights_ref,
    scores_ref,
    changes_ref,
    chances_ref,
    grad_scores_ref,
    encoded_ref,
    grad_ref,
    product_ref,
    pieces_ref,
    queries_ref,
    grads_ref,
    sems,
    out_sems,
    in_sems,
):
    slices, _, rows, _ = pieces_ref.shape
    length = slices * rows
    total, feature = encoded_ref.shape
    width = queries_ref.shape[1]
    blocks = total // length
    tiles = feature // HEAD
    heads = width // HEAD
    spans = blocks // K
    keys = K * length
    scale = HEAD ** (-0.5)
    chunk = 2 * width // (slices * 8)
    tile = 1024
    narrow = range(0, 3 * feature, tile)
    wide = range(0, 2 * width, tile)

    def load(j):
        columns = pl.ds(narrow[j], min(tile, 3 * feature - narrow[j]))
        return pltpu.make_async_copy(
            projection_hbm.at[:, columns], projection_ref.at[:, columns], sems.at[j]
        )

    def wide_load(j):
        columns = pl.ds(wide[j], tile)
        return pltpu.make_async_copy(
            keyvalue_hbm.at[columns], keyvalue_ref.at[columns], sems.at[len(narrow) + 1 + j]
        )

    output_load = pltpu.make_async_copy(output_hbm, output_ref, sems.at[len(narrow)])

    def piece_load(b):
        units = pl.ds(b * tiles, 2 * tiles)
        return pltpu.make_async_copy(
            pieces_hbm.at[:, units], pieces_ref.at[:, units], in_sems.at[2 + b // 2]
        )

    row_loads = [
        pltpu.make_async_copy(queries_hbm, queries_ref, in_sems.at[0]),
        pltpu.make_async_copy(grads_hbm, grads_ref, in_sems.at[1]),
    ]
    piece_load(0).start()
    load(0).start()
    for b in range(2, blocks, 2):
        piece_load(b).start()
    gain = gain_ref[...].reshape(1, feature)
    for b in range(blocks):
        block_rows = slice(b * length, (b + 1) * length)
        if b % 2 == 0:
            piece_load(b).wait()
        for k in range(tiles):
            plain_ref[block_rows, k * HEAD : (k + 1) * HEAD] = (
                pieces_ref[:, b * tiles + k].astype(F32).reshape(length, HEAD)
            )
        normed_ref[block_rows] = rms_norm(plain_ref[block_rows], gain).astype(BF16)

    for j in range(1, len(narrow)):
        load(j).start()
    for j in range(len(narrow)):
        load(j).wait()
        if j == 0:
            output_load.start()
        if j == 1:
            for i in range(len(wide)):
                wide_load(i).start()
            for row_load in row_loads:
                row_load.start()
        columns = slice(narrow[j], min(narrow[j] + tile, 3 * feature))
        qkv_ref[:, columns] = dot(normed_ref[...], projection_ref[:, columns], NN).astype(BF16)

    together = 2
    ones = jnp.ones((length, HEAD), BF16)

    @pl.loop(0, blocks // together)
    def _(step):
        pairs = [(b, h) for b in range(together) for h in range(tiles)]

        def part(which, b, h):
            start = pl.multiple_of((step * together + b) * length, length)
            return qkv_ref[pl.ds(start, length), pl.ds(which * feature + h * HEAD, HEAD)]

        for i, (b, h) in enumerate(pairs):
            encoder_scores_ref[i] = dot(part(0, b, h), part(1, b, h), NT) * scale
        tops = [jnp.max(encoder_scores_ref[i], axis=-1, keepdims=True) for i in range(len(pairs))]
        for i, top in enumerate(tops):
            encoder_weights_ref[i] = jnp.exp(encoder_scores_ref[i] - top).astype(BF16)
        for i, (b, h) in enumerate(pairs):
            value = jnp.concatenate([part(2, b, h), ones], axis=-1)
            summed_up = dot(encoder_weights_ref[i], value, NN)
            start = pl.multiple_of((step * together + b) * length, length)
            mixed_ref[pl.ds(start, length), h * HEAD : (h + 1) * HEAD] = (
                summed_up[:, :HEAD] / summed_up[:, HEAD:]
            ).astype(BF16)

    output_load.wait()
    for start in range(0, feature, 256):
        columns = slice(start, min(start + 256, feature))
        encoded_ref[:, columns] = (
            plain_ref[:, columns] + dot(mixed_ref[...], output_ref[:, columns], NN)
        ).astype(BF16)

    stores = [pltpu.make_async_copy(encoded_ref, encoded_hbm, out_sems.at[0])]
    stores[0].start()
    for j in range(len(wide)):
        wide_load(j).wait()
        columns = slice(wide[j], wide[j] + tile)
        kv_ref[:, columns] = dot(encoded_ref[...], keyvalue_ref[columns, :], NT).astype(BF16)

    for row_load in row_loads:
        row_load.wait()
    key_block = lax.broadcasted_iota(jnp.int32, (1, keys), 1) // length

    @pl.loop(0, spans)
    def _(u):
        valid = key_block < counts_ref[u]
        query_rows = pl.ds(pl.multiple_of(u * SPAN, SPAN), SPAN)
        key_rows = pl.ds(pl.multiple_of(u * keys, keys), keys)

        def columns(h):
            return slice(h * HEAD, (h + 1) * HEAD)

        for h in range(heads):
            key = kv_ref[key_rows, columns(h)]
            value = kv_ref[key_rows, columns(heads + h)]
            scores = dot(queries_ref[query_rows, columns(h)], key, NT) * scale
            scores_ref[h] = jnp.where(valid, scores, -1e30)
            changes_ref[h] = dot(grads_ref[query_rows, columns(h)], value, NT)
        tops = [jnp.max(scores_ref[h], axis=-1, keepdims=True) for h in range(heads)]
        for h in range(heads):
            scores_ref[h] = jnp.exp(scores_ref[h] - tops[h])
        sums = [jnp.sum(scores_ref[h], axis=-1, keepdims=True) for h in range(heads)]
        for h in range(heads):
            chances = scores_ref[h] * (1.0 / sums[h])
            scores_ref[h] = chances
            chances_ref[h] = chances.astype(BF16)
        inners = [
            jnp.sum(scores_ref[h] * changes_ref[h], axis=-1, keepdims=True) for h in range(heads)
        ]
        for h in range(heads):
            grad_scores_ref[h] = (scores_ref[h] * (changes_ref[h] - inners[h])).astype(BF16)
        for h in range(heads):
            value = kv_ref[key_rows, columns(heads + h)]
            query = queries_ref[query_rows, columns(h)]
            grad = grads_ref[query_rows, columns(h)]
            attended_ref[query_rows, columns(h)] = dot(chances_ref[h], value, NN).astype(BF16)
            for part, piece in enumerate(
                (
                    dot(query, grad_scores_ref[h], TN) * scale,
                    dot(grad, chances_ref[h], TN),
                )
            ):
                for j in range(HEAD // 8):
                    row = part * width + h * HEAD + j * 8
                    seq, inside = divmod(row, 8 * chunk)
                    dp, offset = divmod(inside, chunk)
                    base = ((dp // 2) * slices + seq) * chunk + offset
                    grad_ref[dp % 2, base : base + 8, key_rows] = piece[j * 8 : j * 8 + 8].astype(
                        BF16
                    )

    theirs = theirs_ref[0]
    stores.append(pltpu.make_async_copy(grad_ref.at[1 - theirs], own_hbm, out_sems.at[1]))
    stores[1].start()
    for i in range(width // 512):
        part = slice(i * 512, (i + 1) * 512)
        product_ref[part] = dot(grad_ref[theirs, part], encoded_ref[...], NN).astype(BF16)
        stores.append(
            pltpu.make_async_copy(
                product_ref.at[part], product_hbm.at[part], out_sems.at[2 + i]
            )
        )
        stores[-1].start()
    for store in stores:
        store.wait()


def span_step(counts, theirs, pieces, gain, projection, output, keyvalue, queries, grads):
    width = queries.shape[1]
    feature = keyvalue.shape[1]
    slices, units, rows, _ = pieces.shape
    tiles = feature // HEAD
    length = slices * rows
    blocks = units // tiles
    total = blocks * length
    spans = blocks // K
    keys = K * length
    heads = width // HEAD
    whole = pl.BlockSpec(memory_space=VMEM)
    hbm = pl.BlockSpec(memory_space=pltpu.HBM)
    return pl.pallas_call(
        span_kernel,
        out_shape=(
            jax.ShapeDtypeStruct((total, feature), BF16),
            jax.ShapeDtypeStruct((width, total), BF16),
            jax.ShapeDtypeStruct((width, feature), BF16),
            jax.ShapeDtypeStruct((spans * SPAN, width), BF16),
        ),
        in_specs=[
            pl.BlockSpec(memory_space=pltpu.SMEM),
            pl.BlockSpec(memory_space=pltpu.SMEM),
            hbm,
            whole,
            hbm,
            hbm,
            hbm,
            hbm,
            hbm,
        ],
        out_specs=(hbm, hbm, hbm, whole),
        scratch_shapes=[
            VMEM(projection.shape, BF16),
            VMEM(output.shape, BF16),
            VMEM(keyvalue.shape, BF16),
            VMEM((total, feature), F32),
            VMEM((total, feature), BF16),
            VMEM((total, 3 * feature), BF16),
            VMEM((total, feature), BF16),
            VMEM((total, 2 * width), BF16),
            VMEM((2 * tiles, length, length), F32),
            VMEM((2 * tiles, length, length), BF16),
            VMEM((heads, SPAN, keys), F32),
            VMEM((heads, SPAN, keys), F32),
            VMEM((heads, SPAN, keys), BF16),
            VMEM((heads, SPAN, keys), BF16),
            VMEM((total, feature), BF16),
            VMEM((2, width, total), BF16),
            VMEM((width, feature), BF16),
            VMEM(pieces.shape, BF16),
            VMEM(queries.shape, BF16),
            VMEM(queries.shape, BF16),
            pltpu.SemaphoreType.DMA((pl.cdiv(3 * feature, 1024) + 1 + 2 * width // 1024,)),
            pltpu.SemaphoreType.DMA((2 + width // 512,)),
            pltpu.SemaphoreType.DMA((2 + blocks // 2,)),
        ],
        cost_estimate=pl.CostEstimate(
            flops=total * feature * (8 * feature + 6 * width),
            bytes_accessed=20 << 20,
            transcendentals=1 << 20,
        ),
        compiler_params=pltpu.CompilerParams(vmem_limit_bytes=58 << 20),
        name="spans",
    )(counts, theirs, pieces, gain, projection, output, keyvalue, queries, grads)


def weight_kernel(grad_ref, encoded_ref, out_ref):
    out_ref[...] = dot(grad_ref[...], encoded_ref[...], NN).astype(BF16)


def weight_half(grad, encoded):
    rows, keys = grad.shape
    feature = encoded.shape[1]
    tile = 512
    return pl.pallas_call(
        weight_kernel,
        grid=(rows // tile,),
        in_specs=[
            pl.BlockSpec((tile, keys), lambda i: (i, 0)),
            pl.BlockSpec((keys, feature), lambda i: (0, 0)),
        ],
        out_specs=pl.BlockSpec((tile, feature), lambda i: (i, 0)),
        out_shape=jax.ShapeDtypeStruct((rows, feature), BF16),
        cost_estimate=pl.CostEstimate(
            flops=2 * rows * feature * keys, bytes_accessed=8 << 20, transcendentals=0
        ),
        compiler_params=pltpu.CompilerParams(vmem_limit_bytes=24 << 20),
        name="weight_half",
    )(grad, encoded)


def total_kernel(terms_ref, out_ref):
    total = jnp.sum(terms_ref[...].astype(F32), axis=0).astype(BF16)
    for i in range(out_ref.shape[0]):
        out_ref[i] = total


def total_copies(terms, copies):
    whole = pl.BlockSpec(memory_space=VMEM)
    return pl.pallas_call(
        total_kernel,
        out_shape=jax.ShapeDtypeStruct((copies, *terms.shape[1:]), BF16),
        in_specs=[whole],
        out_specs=whole,
        compiler_params=pltpu.CompilerParams(vmem_limit_bytes=16 << 20),
        name="total",
    )(terms)


def all_to_all(block, axis, groups=None):
    return lax.all_to_all(
        block, axis, split_axis=0, concat_axis=0, tiled=True, axis_index_groups=groups
    )


def local(
    hidden,
    database,
    block_home,
    neighbours,
    neighbour_counts,
    encoder_gain,
    encoder_projection,
    encoder_output,
    cross_gain,
    cross_query,
    cross_keyvalue,
    cross_output,
    cotangent,
):
    token_count, _ = hidden.shape
    _, _, feature = database.shape[1:]
    seq = lax.axis_size("seq")
    dp = lax.axis_size("dp")
    requests = neighbours.size
    tail = SPAN - 1

    tiles = feature // HEAD
    slices, tails = spread(block_home, neighbours, database[0], hidden, cotangent, seq)
    late = lax.ppermute(tails, "seq", [(i, i - 1) for i in range(1, seq)])
    late_hidden, late_cotangent = late[0, :tail], late[1, :tail]
    table = all_to_all(slices, "seq")
    readers_where = table[:, -1, 0, :requests].astype(jnp.int32)

    own_hidden = jnp.concatenate([hidden[tail:], late_hidden], axis=0)
    own_cotangent = jnp.concatenate([cotangent[tail:], late_cotangent], axis=0)
    normed = rms_norm(own_hidden, cross_gain).astype(BF16)
    queries = dot(normed, cross_query, NN).astype(BF16)
    grads = dot(own_cotangent, cross_output, NT).astype(BF16)

    picked = pick(readers_where, table, tiles)
    pieces = all_to_all(picked, "seq")
    core = lax.axis_index("dp") % 2
    encoded, own, theirs, attended = span_step(
        neighbour_counts,
        (1 - core).reshape(1),
        pieces,
        encoder_gain,
        encoder_projection,
        encoder_output,
        cross_keyvalue,
        queries,
        grads,
    )
    received = lax.ppermute(theirs, "dp", [(i, i ^ 1) for i in range(dp)])
    mine = weight_half(own, encoded)
    pair = (mine.astype(F32) + received.astype(F32)).astype(BF16)

    half = [
        [d * seq + s for d in range(c, dp, 2) for s in range(seq)] for c in range(2)
    ]
    sent = all_to_all(pair.reshape(dp // 2 * seq, -1, feature), ("dp", "seq"), half)
    keyvalue_grad = all_to_all(total_copies(sent, dp), "dp")
    keyvalue_grad = keyvalue_grad.reshape(-1, feature).astype(F32)

    cross = dot(attended, cross_output, NN)
    rows = (own_hidden.astype(F32) + cross).astype(BF16)
    forth = [(i, i + 1) for i in range(seq - 1)]
    returned = lax.ppermute(rows[token_count - tail :], "seq", forth)
    first = jnp.where(lax.axis_index("seq") == 0, hidden[:tail], returned)
    output = jnp.concatenate([first, rows[: token_count - tail]], axis=0)
    return (output, keyvalue_grad)


def solution(mesh):
    placed = (
        P(("dp", "seq"), None),
        P("dp", "seq", None, None),
        P(),
        P(("dp", "seq"), None),
        P(("dp", "seq")),
        P(),
        P(),
        P(),
        P(),
        P(),
        P(),
        P(),
        P(("dp", "seq"), None),
    )
    return jax.shard_map(
        local,
        mesh=mesh,
        in_specs=placed,
        out_specs=(P(("dp", "seq"), None), P("seq", None)),
        check_vma=False,
    )
```

```python
import functools

import jax
import jax.numpy as jnp
from jax import lax
from jax.experimental import pallas as pl
from jax.experimental.pallas import tpu as pltpu
from jax.sharding import PartitionSpec as P


HEAD = 128
K = 2
SPAN = 64
EPSILON = 1e-06
BF16 = jnp.bfloat16
F32 = jnp.float32
VMEM = pltpu.VMEM
NN = (((1,), (0,)), ((), ()))
NT = (((1,), (1,)), ((), ()))
TN = (((0,), (0,)), ((), ()))


def dot(a, b, dims):
    return lax.dot_general(a, b, dims, preferred_element_type=F32)


def rms_norm(values, norm_gain):
    widened = values.astype(F32)
    return (
        widened
        * lax.rsqrt(jnp.mean(widened * widened, axis=-1, keepdims=True) + EPSILON)
        * norm_gain
    )


def spread_kernel(
    home_ref,
    neighbours_ref,
    blocks_hbm,
    hidden_hbm,
    cotangent_hbm,
    slices_hbm,
    tails_hbm,
    blocks_ref,
    slices_ref,
    tails_ref,
    sems,
    out_sems,
    tail_sems,
):
    blocks, length, feature = blocks_ref.shape
    devices, units, rows, _ = slices_ref.shape
    tiles = feature // HEAD
    parts = sems.shape[0]
    size = length // parts

    def load(part):
        part_rows = pl.ds(part * size, size)
        return pltpu.make_async_copy(
            blocks_hbm.at[:, part_rows], blocks_ref.at[:, part_rows], sems.at[part]
        )

    def store(part):
        several = pl.ds(part * (devices // parts), devices // parts)
        return pltpu.make_async_copy(
            slices_ref.at[several], slices_hbm.at[several], out_sems.at[part]
        )

    span = tails_ref.shape[1]
    tail_loads = [
        pltpu.make_async_copy(rows_hbm.at[pl.ds(0, span)], tails_ref.at[i], tail_sems.at[i])
        for i, rows_hbm in enumerate((hidden_hbm, cotangent_hbm))
    ]
    tail_store = pltpu.make_async_copy(tails_ref, tails_hbm, tail_sems.at[2])
    for part in range(parts):
        load(part).start()
        if part == 0:
            for tail_load in tail_loads:
                tail_load.start()
    lane = lax.broadcasted_iota(jnp.int32, (rows, HEAD), 1)
    notes = jnp.zeros((rows, HEAD), jnp.int32)
    spans, each = neighbours_ref.shape
    for u in range(spans):
        for n in range(each):
            notes = jnp.where(lane == u * each + n, home_ref[neighbours_ref[u, n]], notes)
    notes = notes.astype(F32).astype(BF16)
    for d in range(devices):
        if d % (devices // parts) == 0:
            load(d // (devices // parts)).wait()
        for b in range(blocks):
            for k in range(tiles):
                slices_ref[d, b * tiles + k] = blocks_ref[
                    b, d * rows : (d + 1) * rows, k * HEAD : (k + 1) * HEAD
                ]
        slices_ref[d, units - 1] = notes
        if (d + 1) % (devices // parts) == 0:
            store(d // (devices // parts)).start()
            if d < devices // parts:
                for tail_load in tail_loads:
                    tail_load.wait()
                tail_store.start()
    for part in range(parts):
        store(part).wait()
    tail_store.wait()


def spread(block_home, neighbours, database, hidden, cotangent, devices):
    blocks, length, feature = database.shape
    width = hidden.shape[1]
    units = blocks * (feature // HEAD) + 1
    rows = length // devices
    smem = pl.BlockSpec(memory_space=pltpu.SMEM)
    hbm = pl.BlockSpec(memory_space=pltpu.HBM)
    return pl.pallas_call(
        spread_kernel,
        out_shape=(
            jax.ShapeDtypeStruct((devices, units, rows, HEAD), BF16),
            jax.ShapeDtypeStruct((2, SPAN, width), BF16),
        ),
        in_specs=[smem, smem, hbm, hbm, hbm],
        out_specs=(hbm, hbm),
        scratch_shapes=[
            VMEM(database.shape, BF16),
            VMEM((devices, units, rows, HEAD), BF16),
            VMEM((2, SPAN, width), BF16),
            pltpu.SemaphoreType.DMA((4,)),
            pltpu.SemaphoreType.DMA((4,)),
            pltpu.SemaphoreType.DMA((3,)),
        ],
        cost_estimate=pl.CostEstimate(flops=1 << 20, bytes_accessed=6 << 20, transcendentals=0),
        compiler_params=pltpu.CompilerParams(vmem_limit_bytes=60 << 20),
        name="spread",
    )(block_home, neighbours, database, hidden, cotangent)


def pick_kernel(
    tiles,
    table_hbm,
    out_hbm,
    table_ref,
    notes_ref,
    found_ref,
    where_ref,
    out_ref,
    sems,
    in_sems,
):
    blocks = table_ref.shape[1] // tiles
    parts = sems.shape[0]
    size = out_ref.shape[0] // parts

    def store(part):
        readers = pl.ds(part * size, size)
        return pltpu.make_async_copy(out_ref.at[readers], out_hbm.at[readers], sems.at[part])

    notes_load = pltpu.make_async_copy(
        table_hbm.at[:, table_ref.shape[1] - 1], notes_ref, in_sems.at[0]
    )
    table_load = pltpu.make_async_copy(table_hbm, table_ref, in_sems.at[1])
    notes_load.start()
    table_load.start()
    notes_load.wait()
    found_ref[...] = jnp.max(notes_ref[...].astype(F32), axis=1).astype(jnp.int32)
    where_load = pltpu.make_async_copy(found_ref, where_ref, in_sems.at[2])
    where_load.start()
    where_load.wait()
    table_load.wait()
    for part in range(parts):

        @pl.loop(part * size, (part + 1) * size)
        def _(r):
            for i in range(out_ref.shape[1] // tiles):
                where = where_ref[r, i]
                start = (where % blocks) * tiles
                out_ref[r, i * tiles : (i + 1) * tiles] = table_ref[
                    where // blocks, pl.ds(start, tiles)
                ]

        store(part).start()
    for part in range(parts):
        store(part).wait()


def pick(table, requests, tiles):
    readers, _, rows, width = table.shape
    shape = (readers, requests * tiles, rows, width)
    hbm = pl.BlockSpec(memory_space=pltpu.HBM)
    return pl.pallas_call(
        functools.partial(pick_kernel, tiles),
        out_shape=jax.ShapeDtypeStruct(shape, BF16),
        in_specs=[hbm],
        out_specs=hbm,
        scratch_shapes=[
            VMEM(table.shape, BF16),
            VMEM((readers, rows, width), BF16),
            VMEM((readers, width), jnp.int32),
            pltpu.SMEM((readers, width), jnp.int32),
            VMEM(shape, BF16),
            pltpu.SemaphoreType.DMA((4,)),
            pltpu.SemaphoreType.DMA((3,)),
        ],
        compiler_params=pltpu.CompilerParams(vmem_limit_bytes=60 << 20),
        name="pick",
    )(table)


def span_kernel(
    counts_ref,
    theirs_ref,
    pieces_hbm,
    gain_ref,
    projection_hbm,
    output_hbm,
    keyvalue_hbm,
    queries_hbm,
    grads_hbm,
    encoded_hbm,
    own_hbm,
    product_hbm,
    attended_ref,
    projection_ref,
    output_ref,
    keyvalue_ref,
    plain_ref,
    normed_ref,
    qkv_ref,
    mixed_ref,
    kv_ref,
    encoder_scores_ref,
    encoder_weights_ref,
    scores_ref,
    changes_ref,
    chances_ref,
    grad_scores_ref,
    encoded_ref,
    grad_ref,
    product_ref,
    pieces_ref,
    queries_ref,
    grads_ref,
    sems,
    out_sems,
    in_sems,
):
    slices, _, rows, _ = pieces_ref.shape
    length = slices * rows
    total, feature = encoded_ref.shape
    width = queries_ref.shape[1]
    blocks = total // length
    tiles = feature // HEAD
    heads = width // HEAD
    spans = blocks // K
    keys = K * length
    scale = HEAD ** (-0.5)
    chunk = 2 * width // (slices * 8)
    tile = 1024
    narrow = range(0, 3 * feature, tile)
    wide = range(0, 2 * width, tile)

    def load(j):
        columns = pl.ds(narrow[j], min(tile, 3 * feature - narrow[j]))
        return pltpu.make_async_copy(
            projection_hbm.at[:, columns], projection_ref.at[:, columns], sems.at[j]
        )

    def wide_load(j):
        columns = pl.ds(wide[j], tile)
        return pltpu.make_async_copy(
            keyvalue_hbm.at[columns], keyvalue_ref.at[columns], sems.at[len(narrow) + 1 + j]
        )

    output_load = pltpu.make_async_copy(output_hbm, output_ref, sems.at[len(narrow)])

    def piece_load(b):
        units = pl.ds(b * tiles, 2 * tiles)
        return pltpu.make_async_copy(
            pieces_hbm.at[:, units], pieces_ref.at[:, units], in_sems.at[2 + b // 2]
        )

    row_loads = [
        pltpu.make_async_copy(queries_hbm, queries_ref, in_sems.at[0]),
        pltpu.make_async_copy(grads_hbm, grads_ref, in_sems.at[1]),
    ]
    piece_load(0).start()
    load(0).start()
    for b in range(2, blocks, 2):
        piece_load(b).start()
    gain = gain_ref[...].reshape(1, feature)
    for b in range(blocks):
        block_rows = slice(b * length, (b + 1) * length)
        if b % 2 == 0:
            piece_load(b).wait()
        for k in range(tiles):
            plain_ref[block_rows, k * HEAD : (k + 1) * HEAD] = (
                pieces_ref[:, b * tiles + k].astype(F32).reshape(length, HEAD)
            )
        normed_ref[block_rows] = rms_norm(plain_ref[block_rows], gain).astype(BF16)

    for j in range(1, len(narrow)):
        load(j).start()
    for j in range(len(narrow)):
        load(j).wait()
        if j == 0:
            output_load.start()
        if j == 1:
            for i in range(len(wide)):
                wide_load(i).start()
            for row_load in row_loads:
                row_load.start()
        columns = slice(narrow[j], min(narrow[j] + tile, 3 * feature))
        qkv_ref[:, columns] = dot(normed_ref[...], projection_ref[:, columns], NN).astype(BF16)

    together = 2
    ones = jnp.ones((length, HEAD), BF16)

    @pl.loop(0, blocks // together)
    def _(step):
        pairs = [(b, h) for b in range(together) for h in range(tiles)]

        def part(which, b, h):
            start = pl.multiple_of((step * together + b) * length, length)
            return qkv_ref[pl.ds(start, length), pl.ds(which * feature + h * HEAD, HEAD)]

        for i, (b, h) in enumerate(pairs):
            encoder_scores_ref[i] = dot(part(0, b, h), part(1, b, h), NT) * scale
        tops = [jnp.max(encoder_scores_ref[i], axis=-1, keepdims=True) for i in range(len(pairs))]
        for i, top in enumerate(tops):
            encoder_weights_ref[i] = jnp.exp(encoder_scores_ref[i] - top).astype(BF16)
        for i, (b, h) in enumerate(pairs):
            value = jnp.concatenate([part(2, b, h), ones], axis=-1)
            summed_up = dot(encoder_weights_ref[i], value, NN)
            start = pl.multiple_of((step * together + b) * length, length)
            mixed_ref[pl.ds(start, length), h * HEAD : (h + 1) * HEAD] = (
                summed_up[:, :HEAD] / summed_up[:, HEAD:]
            ).astype(BF16)

    output_load.wait()
    for start in range(0, feature, 256):
        columns = slice(start, min(start + 256, feature))
        encoded_ref[:, columns] = (
            plain_ref[:, columns] + dot(mixed_ref[...], output_ref[:, columns], NN)
        ).astype(BF16)

    stores = [pltpu.make_async_copy(encoded_ref, encoded_hbm, out_sems.at[0])]
    stores[0].start()
    for j in range(len(wide)):
        wide_load(j).wait()
        columns = slice(wide[j], wide[j] + tile)
        kv_ref[:, columns] = dot(encoded_ref[...], keyvalue_ref[columns, :], NT).astype(BF16)

    for row_load in row_loads:
        row_load.wait()
    key_block = lax.broadcasted_iota(jnp.int32, (1, keys), 1) // length

    @pl.loop(0, spans)
    def _(u):
        valid = key_block < counts_ref[u]
        query_rows = pl.ds(pl.multiple_of(u * SPAN, SPAN), SPAN)
        key_rows = pl.ds(pl.multiple_of(u * keys, keys), keys)

        def columns(h):
            return slice(h * HEAD, (h + 1) * HEAD)

        for h in range(heads):
            key = kv_ref[key_rows, columns(h)]
            value = kv_ref[key_rows, columns(heads + h)]
            scores = dot(queries_ref[query_rows, columns(h)], key, NT) * scale
            scores_ref[h] = jnp.where(valid, scores, -1e30)
            changes_ref[h] = dot(grads_ref[query_rows, columns(h)], value, NT)
        tops = [jnp.max(scores_ref[h], axis=-1, keepdims=True) for h in range(heads)]
        for h in range(heads):
            scores_ref[h] = jnp.exp(scores_ref[h] - tops[h])
        sums = [jnp.sum(scores_ref[h], axis=-1, keepdims=True) for h in range(heads)]
        for h in range(heads):
            chances = scores_ref[h] * (1.0 / sums[h])
            scores_ref[h] = chances
            chances_ref[h] = chances.astype(BF16)
        inners = [
            jnp.sum(scores_ref[h] * changes_ref[h], axis=-1, keepdims=True) for h in range(heads)
        ]
        for h in range(heads):
            grad_scores_ref[h] = (scores_ref[h] * (changes_ref[h] - inners[h])).astype(BF16)
        for h in range(heads):
            value = kv_ref[key_rows, columns(heads + h)]
            query = queries_ref[query_rows, columns(h)]
            grad = grads_ref[query_rows, columns(h)]
            attended_ref[query_rows, columns(h)] = dot(chances_ref[h], value, NN).astype(BF16)
            for part, piece in enumerate(
                (
                    dot(query, grad_scores_ref[h], TN) * scale,
                    dot(grad, chances_ref[h], TN),
                )
            ):
                for j in range(HEAD // 8):
                    row = part * width + h * HEAD + j * 8
                    seq, inside = divmod(row, 8 * chunk)
                    dp, offset = divmod(inside, chunk)
                    base = ((dp // 2) * slices + seq) * chunk + offset
                    grad_ref[dp % 2, base : base + 8, key_rows] = piece[j * 8 : j * 8 + 8].astype(
                        BF16
                    )

    theirs = theirs_ref[0]
    stores.append(pltpu.make_async_copy(grad_ref.at[1 - theirs], own_hbm, out_sems.at[1]))
    stores[1].start()
    for i in range(width // 512):
        part = slice(i * 512, (i + 1) * 512)
        product_ref[part] = dot(grad_ref[theirs, part], encoded_ref[...], NN).astype(BF16)
        stores.append(
            pltpu.make_async_copy(
                product_ref.at[part], product_hbm.at[part], out_sems.at[2 + i]
            )
        )
        stores[-1].start()
    for store in stores:
        store.wait()


def span_step(counts, theirs, pieces, gain, projection, output, keyvalue, queries, grads):
    width = queries.shape[1]
    feature = keyvalue.shape[1]
    slices, units, rows, _ = pieces.shape
    tiles = feature // HEAD
    length = slices * rows
    blocks = units // tiles
    total = blocks * length
    spans = blocks // K
    keys = K * length
    heads = width // HEAD
    whole = pl.BlockSpec(memory_space=VMEM)
    hbm = pl.BlockSpec(memory_space=pltpu.HBM)
    return pl.pallas_call(
        span_kernel,
        out_shape=(
            jax.ShapeDtypeStruct((total, feature), BF16),
            jax.ShapeDtypeStruct((width, total), BF16),
            jax.ShapeDtypeStruct((width, feature), BF16),
            jax.ShapeDtypeStruct((spans * SPAN, width), BF16),
        ),
        in_specs=[
            pl.BlockSpec(memory_space=pltpu.SMEM),
            pl.BlockSpec(memory_space=pltpu.SMEM),
            hbm,
            whole,
            hbm,
            hbm,
            hbm,
            hbm,
            hbm,
        ],
        out_specs=(hbm, hbm, hbm, whole),
        scratch_shapes=[
            VMEM(projection.shape, BF16),
            VMEM(output.shape, BF16),
            VMEM(keyvalue.shape, BF16),
            VMEM((total, feature), F32),
            VMEM((total, feature), BF16),
            VMEM((total, 3 * feature), BF16),
            VMEM((total, feature), BF16),
            VMEM((total, 2 * width), BF16),
            VMEM((2 * tiles, length, length), F32),
            VMEM((2 * tiles, length, length), BF16),
            VMEM((heads, SPAN, keys), F32),
            VMEM((heads, SPAN, keys), F32),
            VMEM((heads, SPAN, keys), BF16),
            VMEM((heads, SPAN, keys), BF16),
            VMEM((total, feature), BF16),
            VMEM((2, width, total), BF16),
            VMEM((width, feature), BF16),
            VMEM(pieces.shape, BF16),
            VMEM(queries.shape, BF16),
            VMEM(queries.shape, BF16),
            pltpu.SemaphoreType.DMA((pl.cdiv(3 * feature, 1024) + 1 + 2 * width // 1024,)),
            pltpu.SemaphoreType.DMA((2 + width // 512,)),
            pltpu.SemaphoreType.DMA((2 + blocks // 2,)),
        ],
        cost_estimate=pl.CostEstimate(
            flops=total * feature * (8 * feature + 6 * width),
            bytes_accessed=20 << 20,
            transcendentals=1 << 20,
        ),
        compiler_params=pltpu.CompilerParams(vmem_limit_bytes=58 << 20),
        name="spans",
    )(counts, theirs, pieces, gain, projection, output, keyvalue, queries, grads)


def weight_kernel(grad_ref, encoded_ref, out_ref):
    out_ref[...] = dot(grad_ref[...], encoded_ref[...], NN).astype(BF16)


def weight_half(grad, encoded):
    rows, keys = grad.shape
    feature = encoded.shape[1]
    tile = 512
    return pl.pallas_call(
        weight_kernel,
        grid=(rows // tile,),
        in_specs=[
            pl.BlockSpec((tile, keys), lambda i: (i, 0)),
            pl.BlockSpec((keys, feature), lambda i: (0, 0)),
        ],
        out_specs=pl.BlockSpec((tile, feature), lambda i: (i, 0)),
        out_shape=jax.ShapeDtypeStruct((rows, feature), BF16),
        cost_estimate=pl.CostEstimate(
            flops=2 * rows * feature * keys, bytes_accessed=8 << 20, transcendentals=0
        ),
        compiler_params=pltpu.CompilerParams(vmem_limit_bytes=24 << 20),
        name="weight_half",
    )(grad, encoded)


def total_kernel(terms_ref, out_ref):
    total = jnp.sum(terms_ref[...].astype(F32), axis=0).astype(BF16)
    for i in range(out_ref.shape[0]):
        out_ref[i] = total


def total_copies(terms, copies):
    whole = pl.BlockSpec(memory_space=VMEM)
    return pl.pallas_call(
        total_kernel,
        out_shape=jax.ShapeDtypeStruct((copies, *terms.shape[1:]), BF16),
        in_specs=[whole],
        out_specs=whole,
        compiler_params=pltpu.CompilerParams(vmem_limit_bytes=16 << 20),
        name="total",
    )(terms)


def all_to_all(block, axis, groups=None):
    return lax.all_to_all(
        block, axis, split_axis=0, concat_axis=0, tiled=True, axis_index_groups=groups
    )


def local(
    hidden,
    database,
    block_home,
    neighbours,
    neighbour_counts,
    encoder_gain,
    encoder_projection,
    encoder_output,
    cross_gain,
    cross_query,
    cross_keyvalue,
    cross_output,
    cotangent,
):
    token_count, _ = hidden.shape
    _, _, feature = database.shape[1:]
    seq = lax.axis_size("seq")
    dp = lax.axis_size("dp")
    requests = neighbours.size
    tail = SPAN - 1

    tiles = feature // HEAD
    slices, tails = spread(block_home, neighbours, database[0], hidden, cotangent, seq)
    late = lax.ppermute(tails, "seq", [(i, i - 1) for i in range(1, seq)])
    late_hidden, late_cotangent = late[0, :tail], late[1, :tail]
    table = all_to_all(slices, "seq")

    own_hidden = jnp.concatenate([hidden[tail:], late_hidden], axis=0)
    own_cotangent = jnp.concatenate([cotangent[tail:], late_cotangent], axis=0)
    normed = rms_norm(own_hidden, cross_gain).astype(BF16)
    queries = dot(normed, cross_query, NN).astype(BF16)
    grads = dot(own_cotangent, cross_output, NT).astype(BF16)

    picked = pick(table, requests, tiles)
    pieces = all_to_all(picked, "seq")
    core = lax.axis_index("dp") % 2
    encoded, own, theirs, attended = span_step(
        neighbour_counts,
        (1 - core).reshape(1),
        pieces,
        encoder_gain,
        encoder_projection,
        encoder_output,
        cross_keyvalue,
        queries,
        grads,
    )
    received = lax.ppermute(theirs, "dp", [(i, i ^ 1) for i in range(dp)])
    mine = weight_half(own, encoded)
    pair = (mine.astype(F32) + received.astype(F32)).astype(BF16)

    half = [
        [d * seq + s for d in range(c, dp, 2) for s in range(seq)] for c in range(2)
    ]
    sent = all_to_all(pair.reshape(dp // 2 * seq, -1, feature), ("dp", "seq"), half)
    keyvalue_grad = all_to_all(total_copies(sent, dp), "dp")
    keyvalue_grad = keyvalue_grad.reshape(-1, feature).astype(F32)

    cross = dot(attended, cross_output, NN)
    rows = (own_hidden.astype(F32) + cross).astype(BF16)
    forth = [(i, i + 1) for i in range(seq - 1)]
    returned = lax.ppermute(rows[token_count - tail :], "seq", forth)
    first = jnp.where(lax.axis_index("seq") == 0, hidden[:tail], returned)
    output = jnp.concatenate([first, rows[: token_count - tail]], axis=0)
    return (output, keyvalue_grad)


def solution(mesh):
    placed = (
        P(("dp", "seq"), None),
        P("dp", "seq", None, None),
        P(),
        P(("dp", "seq"), None),
        P(("dp", "seq")),
        P(),
        P(),
        P(),
        P(),
        P(),
        P(),
        P(),
        P(("dp", "seq"), None),
    )
    return jax.shard_map(
        local,
        mesh=mesh,
        in_specs=placed,
        out_specs=(P(("dp", "seq"), None), P("seq", None)),
        check_vma=False,
    )
```
